32 devices in a mesh: dp: 8 (over z, y), mp: 4 (over x, core).
Axes of the slice: x: 2, y: 2, z: 4, core: 2. Of those that a mesh axis runs over, the one named last changes fastest.
Arguments:
- frames: int32 [48], P('dp'), may hold values from 17 to 129, as said below
- owners: int32 [240], P('dp'), may hold values from -1 to 7, as said below
- offsets: int32 [240], P('dp'), may hold values from -1 to 17, as said below
- groups: int32 [48], P('dp'), may hold values from 0 to 3, as said below
- latent: bfloat16 [240, 64, 128], P('dp'), may hold values from -12 to 12
- noise_blocks: bfloat16 [240, 64, 128], P('dp'), may hold values from -6 to 6
- rewards: float32 [48], P('dp'), may hold values from -6 to 6
- embed_weight: bfloat16 [64, 3072], replicated, may hold values from -2 to 2
- norm_gain: float32 [3072], replicated, may hold values from 0 to 2
- mid_weight: bfloat16 [3072, 3072], P(None, 'mp'), may hold values from -1 to 1
- head_weight: bfloat16 [3072, 64], P('mp'), may hold values from -1 to 1
Outputs:
- prediction: bfloat16 [144, 64, 128], P('dp')
- log_prob: float32 [48], P('dp')
- advantage: float32 [48], P('dp')
The draws below stay inside these ranges and needn't reach their ends.
Inputs may be any that keep to these rules, and one draw needn't show every extreme that they name: frames = 4 m + 1 for a whole m; the block counts (frames - 1) // 32 + 1 of all samples add up to exactly 144, and some rollout device has all its samples at 129 frames. `owners`: a live slot names its owner, an empty one -1; every owner receives exactly 18 blocks; one rollout device sends at most 4 blocks to one owner, and in every draw some device sends that many to some owner. `offsets`: a live slot's row at its owner, rows distinct at each owner; empty slots -1. `groups`: every prompt has exactly 12 samples.
All inputs are finite; a program needn't handle non-finite values.
Results may differ from the reference program's by a relative error of at most 0.0068.
Values may be sent and summed in bfloat16 or wider, within the bound.
No kernel may reach another device: no remote copies, remote signals or barrier semaphores. Data moves between devices by JAX's collectives and lax.ppermute only.
A program may use at most 64 MiB of HBM per device.

```python
import math
import jax
import jax.numpy as jnp
from jax import lax

D = 3072
C = 64
BT = 128
MAXB = 5
GSIZE = 12
SPD = 6
SAMPLES = 48
GROUPS = 4
OB = 18
N_DP = 8


def layout(key):
    devices = SAMPLES // SPD
    half_dev = devices // 2
    bias_key = jax.random.fold_in(key, 101)
    shift_key = jax.random.fold_in(key, 102)
    force_key = jax.random.fold_in(key, 103)
    sides_key = jax.random.fold_in(key, 104)
    frame_key = jax.random.fold_in(key, 105)
    order_key = jax.random.fold_in(key, 106)
    device_bias = jax.random.randint(bias_key, (half_dev, 1), -1, 2)
    shifts = jnp.clip(device_bias + jax.random.randint(shift_key, (half_dev, SPD), -1, 2), -2, 2)
    forced = jax.random.randint(force_key, (), 0, half_dev)
    shifts = jnp.where(jnp.arange(half_dev)[:, None] == forced, 2, shifts)
    sides = jax.random.randint(sides_key, (half_dev, 1), 0, 2)
    first_counts = jnp.where(sides == 0, 3 + shifts, 3 - shifts)
    counts = jnp.concatenate([first_counts, 6 - first_counts], axis=0)
    extra_frames = jax.random.randint(frame_key, (devices, SPD), 0, 8)
    latent_minus = jnp.where(counts == 1, jnp.maximum(extra_frames, 4), jnp.where(counts == 5, 32, 8 * (counts - 1) + extra_frames))
    frames = (4 * latent_minus + 1).reshape(-1).astype(jnp.int32)
    live_slot = (jnp.arange(MAXB)[None, None, :] < counts[:, :, None]).astype(jnp.int32)
    live_slot = live_slot.reshape(devices, SPD * MAXB)
    per_dev = jnp.sum(live_slot, axis=1)
    before = jnp.cumsum(per_dev) - per_dev
    within = jnp.cumsum(live_slot, axis=1) - 1
    global_rank = before[:, None] + within
    owner_order = jax.random.permutation(order_key, devices)
    owners = jnp.where(live_slot == 1, jnp.take(owner_order, global_rank % devices), -1)
    offsets = jnp.where(live_slot == 1, global_rank // devices, -1)
    return (frames, owners.reshape(-1).astype(jnp.int32), offsets.reshape(-1).astype(jnp.int32))


def draw_frames(key, part):
    return layout(key)[0]


def draw_owners(key, part):
    return layout(key)[1]


def draw_offsets(key, part):
    return layout(key)[2]


def draw_groups(key, part):
    return (jax.random.permutation(jax.random.fold_in(key, 7), SAMPLES) // GSIZE).astype(jnp.int32)


def base_values(key, shape, bound):
    return jnp.clip(jax.random.normal(key, shape, jnp.float32), -bound, bound)


def model_weights(key):
    embed = base_values(jax.random.fold_in(key, 201), (C, D), 6.0) / math.sqrt(C)
    gain = 1.0 + 0.15 * base_values(jax.random.fold_in(key, 202), (D,), 3.0)
    middle = base_values(jax.random.fold_in(key, 203), (D, D), 6.0) / math.sqrt(D)
    output = base_values(jax.random.fold_in(key, 204), (D, C), 6.0) / math.sqrt(D)
    return (embed, gain, middle, output)


def latent_values(key):
    raw = base_values(jax.random.fold_in(key, 205), (SAMPLES * MAXB, C, BT), 6.0)
    return raw


def rounded(values):
    narrow = lax.optimization_barrier(values.astype(jnp.bfloat16))
    return narrow.astype(jnp.float32)


def draw_latent(key, part):
    return latent_values(key).astype(jnp.bfloat16)


def draw_embed_weight(key, part):
    return model_weights(key)[0].astype(jnp.bfloat16)


def draw_norm_gain(key, part):
    return model_weights(key)[1].astype(jnp.float32)


def draw_mid_weight(key, part):
    return model_weights(key)[2].astype(jnp.bfloat16)


def draw_head_weight(key, part):
    return model_weights(key)[3].astype(jnp.bfloat16)


def draw_noise_blocks(key, part):
    embed, gain, middle, output = model_weights(key)
    embed = rounded(embed)
    middle = rounded(middle)
    output = rounded(output)
    latent = rounded(latent_values(key))

    def one_slot(block):
        embedded = jnp.dot(block.T, embed)
        mean_sq = jnp.mean(embedded * embedded, axis=-1, keepdims=True)
        normed = rounded(embedded / jnp.sqrt(mean_sq + 0.25) * gain)
        activated = rounded(jax.nn.silu(jnp.dot(normed, middle)))
        return jnp.dot(activated, output).T
    velocity = lax.map(one_slot, latent)
    sigma = jnp.exp(jax.random.uniform(jax.random.fold_in(key, 207), (SAMPLES * MAXB, 1, 1), jnp.float32, math.log(0.15), math.log(0.6)))
    fresh = base_values(jax.random.fold_in(key, 208), (SAMPLES * MAXB, C, BT), 6.0)
    return jnp.clip(sigma * fresh - velocity, -6.0, 6.0).astype(jnp.bfloat16)


def levels(rng, shape, split, least, largest):
    level, own = 1.0, jax.random.fold_in(rng, 6)
    for dim, blocks in split:
        heights = jnp.exp(jax.random.uniform(jax.random.fold_in(own, dim), (blocks,), jnp.float32, least / len(split), largest / len(split)))
        level = level * jnp.repeat(heights, shape[dim] // blocks).reshape([-1 if axis == dim else 1 for axis in range(len(shape))])
    return level


def scatter_about(stream_key, extent, spread, limit, shards=(), kind=jnp.bfloat16):
    level = levels(stream_key, extent, shards, -0.22, 0.18) if shards else 1.0
    entries = jax.random.normal(stream_key, extent, jnp.float32) * spread * level
    return jnp.minimum(jnp.maximum(entries, -limit), limit).astype(kind)


def setup_inputs(seed: int = 0) -> dict:
    key_of = jax.random.split(jax.random.key(seed), 12)
    frames = draw_frames(jax.random.fold_in(key_of[11], 71), 0)
    owners = draw_owners(jax.random.fold_in(key_of[11], 71), 0)
    offsets = draw_offsets(jax.random.fold_in(key_of[11], 71), 0)
    groups = draw_groups(jax.random.fold_in(key_of[11], 71), 0)
    latent = draw_latent(jax.random.fold_in(key_of[11], 71), 0)
    noise_blocks = draw_noise_blocks(jax.random.fold_in(key_of[11], 71), 0)
    rewards = scatter_about(key_of[6], (SAMPLES,), 1.0, 6.0, ((0, 8),), jnp.float32)
    embed_weight = draw_embed_weight(jax.random.fold_in(key_of[11], 71), 0)
    norm_gain = draw_norm_gain(jax.random.fold_in(key_of[11], 71), 0)
    mid_weight = draw_mid_weight(jax.random.fold_in(key_of[11], 71), 0)
    head_weight = draw_head_weight(jax.random.fold_in(key_of[11], 71), 0)
    return {"frames": frames, "owners": owners, "offsets": offsets, "groups": groups, "latent": latent, "noise_blocks": noise_blocks, "rewards": rewards, "embed_weight": embed_weight, "norm_gain": norm_gain, "mid_weight": mid_weight, "head_weight": head_weight}


def forward(latent_part, noise_part, embed_weight, norm_gain, mid_weight, head_weight):
    embedded = jnp.einsum('nct,cd->ntd', latent_part.astype(jnp.float32), embed_weight.astype(jnp.float32))
    mean_sq = lax.optimization_barrier(jnp.mean(embedded * embedded, axis=-1, keepdims=True))
    normed = (embedded * lax.rsqrt(mean_sq + 0.25) * norm_gain).astype(jnp.bfloat16)
    mid_out = jnp.einsum('ntd,df->ntf', normed.astype(jnp.float32), mid_weight.astype(jnp.float32))
    activated = jax.nn.silu(mid_out).astype(jnp.bfloat16)
    velocity = jnp.einsum('ntf,fc->nct', activated.astype(jnp.float32), head_weight.astype(jnp.float32))
    errors = noise_part.astype(jnp.float32) + velocity
    return (velocity.astype(jnp.bfloat16), lax.optimization_barrier(jnp.sum(errors * errors, axis=(1, 2))))

def reference(frames, owners, offsets, groups, latent, noise_blocks, rewards, embed_weight, norm_gain, mid_weight, head_weight):
    counts = ((frames - 1) // 32 + 1).astype(jnp.int32)
    slot_index = jnp.arange(SAMPLES * MAXB, dtype=jnp.int32)
    live_slot = slot_index % MAXB < jnp.repeat(counts, MAXB)
    dest_row = jnp.where(live_slot, owners * OB + offsets, N_DP * OB).astype(jnp.int32)
    owner_latent = jnp.zeros((N_DP * OB, C, BT), jnp.bfloat16).at[dest_row].set(latent, mode='drop')
    owner_noise = jnp.zeros((N_DP * OB, C, BT), jnp.bfloat16).at[dest_row].set(noise_blocks, mode='drop')
    sample_ids = (slot_index // MAXB).astype(jnp.int32)
    owner_sample = jnp.zeros((N_DP * OB,), jnp.int32).at[dest_row].set(sample_ids, mode='drop')

    def per_owner(pieces):
        return forward(pieces[0], pieces[1], embed_weight, norm_gain, mid_weight, head_weight)
    preds, slot_sums = lax.map(per_owner, (owner_latent.reshape(N_DP, OB, C, BT), owner_noise.reshape(N_DP, OB, C, BT)))
    prediction = preds.reshape(N_DP * OB, C, BT)
    totals = jax.ops.segment_sum(slot_sums.reshape(-1), owner_sample, num_segments=SAMPLES)
    log_prob = -0.5 * totals / (counts * BT * C).astype(jnp.float32)
    group_sum = jax.ops.segment_sum(rewards, groups, num_segments=GROUPS)
    group_sq = jax.ops.segment_sum(rewards * rewards, groups, num_segments=GROUPS)
    group_mean = group_sum / GSIZE
    variance = group_sq / GSIZE - group_mean * group_mean
    advantage = (rewards - group_mean[groups]) / jnp.sqrt(variance[groups] + 0.25)
    return (prediction, log_prob, advantage)
```

```python
import functools

import jax
import jax.numpy as jnp
from jax import lax
from jax.experimental import pallas as pl
from jax.experimental.pallas import tpu as pltpu
from jax.sharding import PartitionSpec as P

GSIZE = 12
META = 16
LANES = 128
F32 = jnp.float32
BF16 = jnp.bfloat16
SMEM = pl.BlockSpec(memory_space=pltpu.SMEM)
VMEM = pl.BlockSpec(memory_space=pltpu.VMEM)
ANY = pl.BlockSpec(memory_space=pl.ANY)


def split3(value):
    hi = value.astype(BF16)
    rest = value - hi.astype(F32)
    mid = rest.astype(BF16)
    lo = (rest - mid.astype(F32)).astype(BF16)
    return hi, mid, lo


def lane_row(scalars, count, dtype):
    lane = lax.broadcasted_iota(jnp.int32, (1, LANES), 1)
    row = jnp.zeros((1, LANES), dtype)
    for s in range(count):
        row = jnp.where(lane == s, scalars(s), row)
    return row


def live_count(frames, sample):
    return lax.shift_right_logical(frames[sample] - 1, 5) + 1


def pack_kernel(maxb, per_pair, mp, frames, owners, offsets, groups, rewards, latent, send, places, rows, sems):
    peers = send.shape[0]
    channels = latent.shape[1]
    slots = owners.shape[0]
    shift = lax.axis_index("mp") + mp - lax.rem(lax.axis_index("dp"), mp)
    for o in range(peers):
        places[o] = 0
        for q in range(per_pair):
            rows[o * per_pair + q] = 0
    for i in range(slots):
        o = jnp.maximum(owners[i], 0)
        live = (i % maxb) < live_count(frames, i // maxb)
        place = places[o]
        q = place // mp
        mine = live & (lax.rem(place - lax.rem(shift, mp) + mp, mp) == 0) & (q < per_pair)

        @pl.when(live)
        def _():
            places[o] = place + 1

        @pl.when(mine)
        def _():
            rows[o * per_pair + q] = offsets[i] + 1
            pltpu.make_async_copy(
                latent.at[i], send.at[o, pl.ds(q * channels, channels)], sems.at[o * per_pair + q]
            ).start()

    samples = frames.shape[0]
    hi, mid, lo = split3(lane_row(lambda s: rewards[s], samples, F32))
    group = lane_row(lambda s: groups[s].astype(F32), samples, F32)
    sub = lax.broadcasted_iota(jnp.int32, (META, LANES), 0)
    shared = jnp.where(sub == 1, hi.astype(F32), 0.0)
    shared = jnp.where(sub == 2, mid.astype(F32), shared)
    shared = jnp.where(sub == 3, lo.astype(F32), shared)
    shared = jnp.where(sub == 4, group, shared)
    for o in range(peers):
        first = lane_row(lambda q: rows[o * per_pair + q].astype(F32), per_pair, F32)
        send[o, pl.ds(per_pair * channels, META), :] = jnp.where(sub == 0, first, shared).astype(BF16)
    for o in range(peers):
        for q in range(per_pair):
            n = o * per_pair + q

            @pl.when(rows[n] > 0)
            def _():
                pltpu.make_async_copy(
                    latent.at[0], send.at[o, pl.ds(q * channels, channels)], sems.at[n]
                ).wait()


def combine_kernel(step, embed, gain, weight, head, out, gram, held, sems):
    channels = embed.shape[0]
    hidden = weight.shape[1]
    copies = [
        pltpu.make_async_copy(weight.at[:, pl.ds(n, step)], held.at[:, pl.ds(n, step)], sems.at[n // step])
        for n in range(0, hidden, step)
    ]
    for copy in copies:
        copy.start()
    out[channels:, :] = head[...].T
    e = embed[...]
    hi, mid, lo = split3(lax.dot_general(e, e, (((1,), (1,)), ((), ())), preferred_element_type=F32))
    gram[...] = jnp.concatenate([hi, mid, lo], axis=0)
    scaled = e.astype(F32) * gain[...]
    hi = scaled.astype(BF16)
    lo = (scaled - hi.astype(F32)).astype(BF16)
    both = jnp.concatenate([hi, lo], axis=0)
    for n, copy in enumerate(copies):
        copy.wait()
        m = jnp.dot(both, held[:, n * step : (n + 1) * step], preferred_element_type=F32)
        out[:channels, n * step : (n + 1) * step] = (m[:channels] + m[channels:]).astype(BF16)


def velocity(x, mt, both, features):
    shards, two, hidden = both.shape
    channels = two // 2
    tall = shards * hidden
    g = jnp.dot(mt[tall:, :], x, preferred_element_type=F32)
    gx = g[:channels] + g[channels : 2 * channels] + g[2 * channels :]
    mean_sq = jnp.sum(gx * x.astype(F32), axis=0, keepdims=True) * (1.0 / features)
    half = 0.5 * lax.rsqrt(jnp.maximum(mean_sq, 0.0) + 0.25)
    step = 256
    total = None
    for m in range(shards):
        for h in range(0, hidden, step):
            mid = jnp.dot(mt[m * hidden + h : m * hidden + h + step, :], x, preferred_element_type=F32)
            v = mid * half
            act = (v + v * jnp.tanh(v)).astype(BF16)
            part = jnp.dot(both[m, channels:, h : h + step], act, preferred_element_type=F32)
            total = part if total is None else total + part
    return total


def errors_kernel(maxb, mp, features, frames, latent, noise, both, gram, errs, mt, sems_list, acc):
    shards, two, hidden = both.shape
    channels = two // 2
    width = latent.shape[2]
    for m in range(shards):
        mt[m * hidden : (m + 1) * hidden, :] = both[m, :channels, :].T
    mt[shards * hidden :, :] = gram[...]
    me = lax.axis_index("mp")
    seen = jnp.int32(0)
    count = jnp.int32(0)
    for i in range(latent.shape[0]):
        live = (i % maxb) < live_count(frames, i // maxb)
        mine = live & (lax.rem(seen, mp) == me)

        @pl.when(mine)
        def _():
            sems_list[count] = i

        seen = seen + live.astype(jnp.int32)
        count = count + mine.astype(jnp.int32)
    acc[...] = jnp.zeros_like(acc)

    def body(pair, carry):
        first = sems_list[2 * pair]
        more = 2 * pair + 1 < count
        second = jnp.where(more, sems_list[2 * pair + 1], first)
        x = jnp.concatenate([latent[first], latent[second]], axis=1)
        v = velocity(x, mt, both, features)
        e = jnp.concatenate([noise[first], noise[second]], axis=1).astype(F32) + v
        rows = jnp.sum(e * e, axis=0, keepdims=True)
        s0 = first // maxb
        acc[pl.ds(s0, 1), :] += rows[:, :width]

        @pl.when(more)
        def _():
            acc[pl.ds(second // maxb, 1), :] += rows[:, width:]

        return carry

    lax.fori_loop(0, (count + 1) // 2, body, 0)
    sums = jnp.sum(acc[...], axis=1, keepdims=True)
    lane = lax.broadcasted_iota(jnp.int32, acc.shape, 1)
    sub = lax.broadcasted_iota(jnp.int32, acc.shape, 0)
    errs[...] = jnp.sum(jnp.where(lane == sub, sums, 0.0), axis=0, keepdims=True)


def owner_kernel(per_pair, features, recv, errs, both, mt, out, table_v, table, order, sem):
    peers = recv.shape[0]
    channels = both.shape[1] // 2
    total = peers * per_pair
    table_v[...] = recv[:, per_pair * channels, :].astype(F32).astype(jnp.int32)
    copy = pltpu.make_async_copy(table_v, table, sem)
    copy.start()
    copy.wait()
    count = jnp.int32(0)
    for d in range(peers):
        for q in range(per_pair):
            live = table[d, q] > 0

            @pl.when(live)
            def _():
                order[count] = d * per_pair + q

            count = count + live.astype(jnp.int32)

    def body(pair, carry):
        first = order[2 * pair]
        more = 2 * pair + 1 < count
        second = jnp.where(more, order[2 * pair + 1], first)
        x = jnp.concatenate(
            [
                recv[n // per_pair, pl.ds(pl.multiple_of((n % per_pair) * channels, channels), channels), :]
                for n in (first, second)
            ],
            axis=1,
        )
        v = velocity(x, mt, both, features).astype(BF16)
        width = v.shape[1] // 2
        out[pl.ds(pl.multiple_of(2 * pair * channels, channels), channels), :] = v[:, :width]
        out[pl.ds(pl.multiple_of((2 * pair + 1) * channels, channels), channels), :] = v[:, width:]
        return carry

    lax.fori_loop(0, (count + 1) // 2, body, 0)
    lane = lax.broadcasted_iota(jnp.int32, (1, LANES), 1)

    def put(j, row):
        n = order[jnp.minimum(j, jnp.maximum(count - 1, 0))]
        value = table[n // per_pair, n % per_pair]
        return jnp.where((lane == j) & (j < count), value.astype(F32), row)

    order[total] = 0

    @pl.when(count == 0)
    def _():
        order[0] = 0

    first = lax.fori_loop(0, total, put, jnp.zeros((1, LANES), F32))
    hi, mid, lo = split3(errs[...])
    sub = lax.broadcasted_iota(jnp.int32, (META, LANES), 0)
    meta = jnp.where(sub == 0, first, 0.0)
    meta = jnp.where(sub == 1, hi.astype(F32), meta)
    meta = jnp.where(sub == 2, mid.astype(F32), meta)
    meta = jnp.where(sub == 3, lo.astype(F32), meta)
    out[total * channels :, :] = meta.astype(BF16)


def place_kernel(per_pair, frames, groups, rewards, recv, gathered, pred, log_prob, advantage, table_v, table, sems, sem):
    shards = gathered.shape[0]
    channels = pred.shape[1]
    block = pred.shape[1] * pred.shape[2]
    total = (gathered.shape[1] - META) // channels
    samples = frames.shape[0]
    base = total * channels
    table_v[...] = gathered[:, base, :].astype(F32).astype(jnp.int32)
    copy = pltpu.make_async_copy(table_v, table, sem)
    copy.start()
    copy.wait()

    def each(act):
        def body(j, carry):
            for m in range(shards):
                row = table[m, j]

                @pl.when(row > 0)
                def _():
                    act(
                        pltpu.make_async_copy(
                            gathered.at[m, pl.ds(pl.multiple_of(j * channels, channels), channels)],
                            pred.at[row - 1],
                            sems.at[m * total + j],
                        )
                    )

            return carry

        lax.fori_loop(0, total, body, 0)

    each(lambda c: c.start())

    lane = lax.broadcasted_iota(jnp.int32, (1, LANES), 1)
    sums = jnp.zeros((1, LANES), F32)
    for m in range(shards):
        part = gathered[m, pl.ds(base, META), :].astype(F32)
        sums = sums + (part[1:2] + part[2:3] + part[3:4])
    size = lane_row(lambda s: (live_count(frames, s) * block).astype(F32), samples, F32)
    logs = -0.5 * sums / jnp.where(lane < samples, size, 1.0)

    info = recv[:, pl.ds(per_pair * channels, META), :].astype(F32)
    every = info[:, 1, :] + info[:, 2, :] + info[:, 3, :]
    group = info[:, 4, :]
    inside = lax.broadcasted_iota(jnp.int32, every.shape, 1) < samples
    for s in range(samples):
        chosen = inside & (group == groups[s].astype(F32))
        mean = jnp.sum(jnp.where(chosen, every, 0.0), keepdims=True) / GSIZE
        meansq = jnp.sum(jnp.where(chosen, every * every, 0.0), keepdims=True) / GSIZE
        value = (rewards[s] - mean) / jnp.sqrt(meansq - mean * mean + 0.25)
        advantage[s] = jnp.sum(value)
        log_prob[s] = jnp.sum(jnp.where(lane == s, logs, 0.0))
    each(lambda c: c.wait())


def local(
    frames,
    owners,
    offsets,
    groups,
    latent,
    noise_blocks,
    rewards,
    embed_weight,
    norm_gain,
    mid_weight,
    head_weight,
):
    samples = frames.shape[0]
    slots, channels, width = latent.shape
    maxb = slots // samples
    peers = lax.axis_size("dp")
    mp = lax.axis_size("mp")
    features, hidden = mid_weight.shape
    pair_cap = (slots + peers - 1) // peers
    per_pair = (pair_cap + mp - 1) // mp
    total = peers * per_pair
    owner_rows = 3 * samples
    tall = mp * hidden + 3 * channels
    params = functools.partial(pltpu.CompilerParams, vmem_limit_bytes=48 * 1024 * 1024)

    step = next(n for n in (256, 128, hidden) if hidden % n == 0)
    combined, gram = pl.pallas_call(
        functools.partial(combine_kernel, step),
        in_specs=[VMEM, VMEM, ANY, VMEM],
        out_specs=[VMEM, VMEM],
        out_shape=[
            jax.ShapeDtypeStruct((2 * channels, hidden), BF16),
            jax.ShapeDtypeStruct((3 * channels, channels), BF16),
        ],
        scratch_shapes=[
            pltpu.VMEM((features, hidden), BF16),
            pltpu.SemaphoreType.DMA((hidden // step,)),
        ],
        compiler_params=params(),
        name="combine",
    )(embed_weight, norm_gain.reshape(1, features), mid_weight, head_weight)

    send = pl.pallas_call(
        functools.partial(pack_kernel, maxb, per_pair, mp),
        in_specs=[SMEM] * 5 + [ANY],
        out_specs=VMEM,
        out_shape=jax.ShapeDtypeStruct((peers, per_pair * channels + META, width), BF16),
        scratch_shapes=[
            pltpu.SMEM((peers,), jnp.int32),
            pltpu.SMEM((total,), jnp.int32),
            pltpu.SemaphoreType.DMA((total,)),
        ],
        compiler_params=params(),
        name="pack",
    )(frames, owners, offsets, groups, rewards, latent)

    recv = lax.all_to_all(send, "dp", split_axis=0, concat_axis=0, tiled=True)
    both = lax.all_gather(combined, "mp", axis=0, tiled=False)

    rows8 = (samples + 7) // 8 * 8
    errs, mt = pl.pallas_call(
        functools.partial(errors_kernel, maxb, mp, features),
        in_specs=[SMEM] + [VMEM] * 4,
        out_specs=[VMEM, VMEM],
        out_shape=[
            jax.ShapeDtypeStruct((1, LANES), F32),
            jax.ShapeDtypeStruct((tall, channels), BF16),
        ],
        scratch_shapes=[pltpu.SMEM((slots + 2,), jnp.int32), pltpu.VMEM((rows8, width), F32)],
        compiler_params=params(),
        name="errors",
    )(frames, latent, noise_blocks, both, gram)

    payload = pl.pallas_call(
        functools.partial(owner_kernel, per_pair, features),
        in_specs=[VMEM] * 4,
        out_specs=VMEM,
        out_shape=jax.ShapeDtypeStruct((((total + 1) // 2 * 2) * channels + META, width), BF16),
        scratch_shapes=[
            pltpu.VMEM((peers, LANES), jnp.int32),
            pltpu.SMEM((peers, LANES), jnp.int32),
            pltpu.SMEM((total + 2,), jnp.int32),
            pltpu.SemaphoreType.DMA,
        ],
        compiler_params=params(),
        name="owner",
    )(recv, errs, both, mt)

    gathered = lax.all_gather(payload, "mp", axis=0, tiled=False)

    return pl.pallas_call(
        functools.partial(place_kernel, per_pair),
        in_specs=[SMEM] * 3 + [VMEM, VMEM],
        out_specs=[ANY, SMEM, SMEM],
        out_shape=[
            jax.ShapeDtypeStruct((owner_rows, channels, width), BF16),
            jax.ShapeDtypeStruct((samples,), F32),
            jax.ShapeDtypeStruct((samples,), F32),
        ],
        scratch_shapes=[
            pltpu.VMEM((mp, LANES), jnp.int32),
            pltpu.SMEM((mp, LANES), jnp.int32),
            pltpu.SemaphoreType.DMA((mp * total,)),
            pltpu.SemaphoreType.DMA,
        ],
        compiler_params=params(),
        name="place",
    )(frames, groups, rewards, recv, gathered)


def solution(mesh):
    placed = (
        P("dp"),
        P("dp"),
        P("dp"),
        P("dp"),
        P("dp", None, None),
        P("dp", None, None),
        P("dp"),
        P(),
        P(),
        P(None, "mp"),
        P("mp", None),
    )
    return jax.shard_map(
        local,
        mesh=mesh,
        in_specs=placed,
        out_specs=(P("dp", None, None), P("dp"), P("dp")),
        check_vma=False,
    )
```

```python
import functools

import jax
import jax.numpy as jnp
from jax import lax
from jax.experimental import pallas as pl
from jax.experimental.pallas import tpu as pltpu
from jax.sharding import PartitionSpec as P

GSIZE = 12
META = 16
LANES = 128
F32 = jnp.float32
BF16 = jnp.bfloat16
SMEM = pl.BlockSpec(memory_space=pltpu.SMEM)
VMEM = pl.BlockSpec(memory_space=pltpu.VMEM)
ANY = pl.BlockSpec(memory_space=pl.ANY)
HBM = pl.BlockSpec(memory_space=pltpu.HBM)


def in_hbm(value):
    return pltpu.with_memory_space_constraint(value, pltpu.HBM)


def split3(value):
    hi = value.astype(BF16)
    rest = value - hi.astype(F32)
    mid = rest.astype(BF16)
    lo = (rest - mid.astype(F32)).astype(BF16)
    return hi, mid, lo


def lane_row(scalars, count, dtype):
    lane = lax.broadcasted_iota(jnp.int32, (1, LANES), 1)
    row = jnp.zeros((1, LANES), dtype)
    for s in range(count):
        row = jnp.where(lane == s, scalars(s), row)
    return row


def live_count(frames, sample):
    return lax.shift_right_logical(frames[sample] - 1, 5) + 1


def start_kernel(
    maxb,
    per_pair,
    mp,
    step,
    frames_h,
    owners_h,
    offsets_h,
    groups_h,
    rewards_h,
    latent,
    noise,
    embed_h,
    gain_h,
    weight,
    head_h,
    out,
    gram,
    send,
    block_x,
    block_n,
    picks,
    frames,
    owners,
    offsets,
    groups,
    rewards,
    embed,
    gain,
    held,
    places,
    rows,
    chosen,
    small_sems,
    big_sems,
    weight_sems,
    row_sems,
    x_sems,
    n_sems,
):
    peers = send.shape[0]
    _, channels, width = latent.shape
    hidden = weight.shape[1]
    samples = frames.shape[0]
    share = block_x.shape[0] * 2
    small = [
        pltpu.make_async_copy(a, b, small_sems.at[n])
        for n, (a, b) in enumerate(
            [
                (frames_h, frames),
                (owners_h, owners),
                (offsets_h, offsets),
                (groups_h, groups),
                (rewards_h, rewards),
            ]
        )
    ]
    big = [
        pltpu.make_async_copy(embed_h, embed, big_sems.at[0]),
        pltpu.make_async_copy(gain_h, gain, big_sems.at[1]),
        pltpu.make_async_copy(head_h, out.at[pl.ds(channels, channels)], big_sems.at[2]),
    ]
    parts = [
        pltpu.make_async_copy(weight.at[:, pl.ds(n, step)], held.at[:, pl.ds(n, step)], weight_sems.at[n // step])
        for n in range(0, hidden, step)
    ]
    for copy in small + big + parts:
        copy.start()
    for copy in small:
        copy.wait()

    def pick(source, target, sems, i, j):
        half = pl.multiple_of(lax.rem(j, 2) * width, width)
        return pltpu.make_async_copy(source.at[i], target.at[j // 2, :, pl.ds(half, width)], sems.at[j])

    def block(o, q, i):
        return pltpu.make_async_copy(latent.at[i], send.at[o, pl.ds(q * channels, channels)], row_sems.at[o * per_pair + q])

    me = lax.axis_index("mp")
    shift = lax.rem(me + mp - lax.rem(lax.axis_index("dp"), mp), mp)
    for o in range(peers):
        places[o] = 0
        for q in range(per_pair):
            rows[o * per_pair + q] = 0
    seen = jnp.int32(0)
    count = jnp.int32(0)
    for s in range(samples):
        live_here = live_count(frames, s)
        for k in range(maxb):
            i = s * maxb + k
            live = k < live_here
            o = jnp.maximum(owners[i], 0)
            place = places[o]
            q = place // mp
            sends = live & (lax.rem(place, mp) == shift) & (q < per_pair)
            mine = live & (lax.rem(seen, mp) == me)

            @pl.when(live)
            def _():
                places[o] = place + 1

            @pl.when(sends)
            def _():
                rows[o * per_pair + q] = offsets[i] + 1
                block(o, q, i).start()

            @pl.when(mine)
            def _():
                chosen[count] = s
                pick(latent, block_x, x_sems, i, count).start()
                pick(noise, block_n, n_sems, i, count).start()

            seen = seen + live.astype(jnp.int32)
            count = count + mine.astype(jnp.int32)

    lane = lax.broadcasted_iota(jnp.int32, (1, LANES), 1)
    found = jnp.where(lane == LANES - 1, count, 0)
    for j in range(share):
        found = jnp.where((lane == j) & (j < count), chosen[j], found)
    picks[...] = found

    hi, mid, lo = split3(lane_row(lambda s: rewards[s], samples, F32))
    group = lane_row(lambda s: groups[s].astype(F32), samples, F32)
    sub = lax.broadcasted_iota(jnp.int32, (META, LANES), 0)
    shared = jnp.where(sub == 1, hi.astype(F32), 0.0)
    shared = jnp.where(sub == 2, mid.astype(F32), shared)
    shared = jnp.where(sub == 3, lo.astype(F32), shared)
    shared = jnp.where(sub == 4, group, shared)
    for o in range(peers):
        first = lane_row(lambda q: rows[o * per_pair + q].astype(F32), per_pair, F32)
        send[o, pl.ds(per_pair * channels, META), :] = jnp.where(sub == 0, first, shared).astype(BF16)

    big[0].wait()
    e = embed[...]
    hi, mid, lo = split3(lax.dot_general(e, e, (((1,), (1,)), ((), ())), preferred_element_type=F32))
    gram[...] = jnp.concatenate([hi, mid, lo], axis=0)
    big[1].wait()
    scaled = e.astype(F32) * gain[...]
    hi = scaled.astype(BF16)
    lo = (scaled - hi.astype(F32)).astype(BF16)
    both = jnp.concatenate([hi, lo], axis=0)
    for n, copy in enumerate(parts):
        copy.wait()
        m = jnp.dot(both, held[:, n * step : (n + 1) * step], preferred_element_type=F32)
        out[:channels, n * step : (n + 1) * step] = (m[:channels] + m[channels:]).astype(BF16)
    big[2].wait()
    for o in range(peers):
        for q in range(per_pair):

            @pl.when(rows[o * per_pair + q] > 0)
            def _():
                block(o, q, 0).wait()

    for j in range(share):

        @pl.when(j < count)
        def _():
            pick(latent, block_x, x_sems, 0, j).wait()
            pick(noise, block_n, n_sems, 0, j).wait()


def velocity(x, mt, heads, features):
    channels, hidden = heads[0].shape[0] // 2, heads[0].shape[1]
    tall = len(heads) * hidden
    g = jnp.dot(mt[tall:, :], x, preferred_element_type=F32)
    gx = g[:channels] + g[channels : 2 * channels] + g[2 * channels :]
    mean_sq = jnp.sum(gx * x.astype(F32), axis=0, keepdims=True) * (1.0 / features)
    half = 0.5 * lax.rsqrt(jnp.maximum(mean_sq, 0.0) + 0.25)
    step = next(n for n in (256, 128, hidden) if hidden % n == 0)
    total = None
    for m, head in enumerate(heads):
        for h in range(0, hidden, step):
            mid = jnp.dot(mt[m * hidden + h : m * hidden + h + step, :], x, preferred_element_type=F32)
            v = mid * half
            act = (v + v * jnp.tanh(v)).astype(BF16)
            part = jnp.dot(head[channels:, h : h + step], act, preferred_element_type=F32)
            total = part if total is None else total + part
    return total


def errors_kernel(shards, features, picks, block_x, block_n, gram, *refs):
    heads, (errs, mt, acc, table, sem) = refs[:shards], refs[shards:]
    channels, hidden = heads[0].shape[0] // 2, heads[0].shape[1]
    width = block_x.shape[2] // 2
    copy = pltpu.make_async_copy(picks, table, sem)
    copy.start()
    for m, head in enumerate(heads):
        mt[m * hidden : (m + 1) * hidden, :] = head[:channels, :].T
    mt[shards * hidden :, :] = gram[...]
    acc[...] = jnp.zeros_like(acc)
    copy.wait()
    count = table[0, LANES - 1]

    def body(pair, carry):
        v = velocity(block_x[pair], mt, heads, features)
        e = block_n[pair].astype(F32) + v
        rows = jnp.sum(e * e, axis=0, keepdims=True)
        acc[pl.ds(table[0, 2 * pair], 1), :] += rows[:, :width]

        @pl.when(2 * pair + 1 < count)
        def _():
            acc[pl.ds(table[0, 2 * pair + 1], 1), :] += rows[:, width:]

        return carry

    lax.fori_loop(0, (count + 1) // 2, body, 0)
    sums = jnp.sum(acc[...], axis=1, keepdims=True)
    lane = lax.broadcasted_iota(jnp.int32, acc.shape, 1)
    sub = lax.broadcasted_iota(jnp.int32, acc.shape, 0)
    errs[...] = jnp.sum(jnp.where(lane == sub, sums, 0.0), axis=0, keepdims=True)


def owner_kernel(per_pair, shards, features, recv, errs, mt, *refs):
    heads, (out, order) = refs[:shards], refs[shards:]
    peers = recv.shape[0]
    channels = heads[0].shape[0] // 2
    total = peers * per_pair
    base = total * channels
    first = recv[:, per_pair * channels, :].astype(F32)
    out[base : base + peers, :] = first.astype(BF16)
    lane = lax.broadcasted_iota(jnp.int32, (peers, LANES), 1)
    number = lax.broadcasted_iota(jnp.int32, (peers, LANES), 0) * per_pair + lane
    count = jnp.int32(0)
    for low in range(0, total, 16):
        inside = (lane < per_pair) & (number >= low) & (number < low + 16) & (first > 0)
        bits = jnp.where(inside, lax.shift_left(1, jnp.clip(number - low, 0, 15)).astype(F32), 0.0)
        mask = jnp.sum(bits).astype(jnp.int32)
        for n in range(low, min(low + 16, total)):
            live = lax.bitwise_and(lax.shift_right_logical(mask, n - low), 1)

            @pl.when(live > 0)
            def _():
                order[count] = n

            count = count + live

    def body(pair, carry):
        one = order[2 * pair]
        more = 2 * pair + 1 < count
        two = jnp.where(more, order[2 * pair + 1], one)
        x = jnp.concatenate(
            [
                recv[n // per_pair, pl.ds(pl.multiple_of((n % per_pair) * channels, channels), channels), :]
                for n in (one, two)
            ],
            axis=1,
        )
        v = velocity(x, mt, heads, features).astype(BF16)
        width = v.shape[1] // 2
        out[pl.ds(pl.multiple_of(one * channels, channels), channels), :] = v[:, :width]

        @pl.when(more)
        def _():
            out[pl.ds(pl.multiple_of(two * channels, channels), channels), :] = v[:, width:]

        return carry

    lax.fori_loop(0, (count + 1) // 2, body, 0)
    hi, mid, lo = split3(errs[...])
    sub = lax.broadcasted_iota(jnp.int32, (META, LANES), 0)
    meta = jnp.where(sub == 0, hi.astype(F32), 0.0)
    meta = jnp.where(sub == 1, mid.astype(F32), meta)
    meta = jnp.where(sub == 2, lo.astype(F32), meta)
    out[out.shape[0] - META :, :] = meta.astype(BF16)


def place_kernel(
    per_pair,
    frames_h,
    groups_h,
    rewards_h,
    recv,
    gathered,
    pred,
    log_prob,
    advantage,
    frames,
    groups,
    rewards,
    table_v,
    table,
    small_sems,
    sems,
    sem,
):
    shards = gathered.shape[0]
    channels = pred.shape[1]
    block = pred.shape[1] * pred.shape[2]
    peers = recv.shape[0]
    total = peers * per_pair
    samples = frames.shape[0]
    base = total * channels
    small = [
        pltpu.make_async_copy(a, b, small_sems.at[n])
        for n, (a, b) in enumerate([(frames_h, frames), (groups_h, groups), (rewards_h, rewards)])
    ]
    for copy in small:
        copy.start()
    for m in range(shards):
        table_v[m * peers : (m + 1) * peers, :] = gathered[m, base : base + peers, :].astype(F32).astype(jnp.int32)
    copy = pltpu.make_async_copy(table_v, table, sem)
    copy.start()
    for one in small:
        one.wait()
    copy.wait()

    def each(act):
        def body(d, carry):
            for m in range(shards):
                for q in range(per_pair):
                    row = table[m * peers + d, q]
                    n = d * per_pair + q

                    @pl.when(row > 0)
                    def _():
                        act(
                            pltpu.make_async_copy(
                                gathered.at[m, pl.ds(pl.multiple_of(n * channels, channels), channels)],
                                pred.at[row - 1],
                                sems.at[m * total + n],
                            )
                        )

            return carry

        lax.fori_loop(0, peers, body, 0, unroll=peers <= 8)

    each(lambda c: c.start())

    lane = lax.broadcasted_iota(jnp.int32, (1, LANES), 1)
    sums = jnp.zeros((1, LANES), F32)
    for m in range(shards):
        part = gathered[m, gathered.shape[1] - META :, :].astype(F32)
        sums = sums + (part[0:1] + part[1:2] + part[2:3])
    size = lane_row(lambda s: (live_count(frames, s) * block).astype(F32), samples, F32)
    logs = -0.5 * sums / jnp.where(lane < samples, size, 1.0)

    info = recv[:, pl.ds(per_pair * channels, META), :].astype(F32)
    every = info[:, 1, :] + info[:, 2, :] + info[:, 3, :]
    group = info[:, 4, :]
    inside = lax.broadcasted_iota(jnp.int32, every.shape, 1) < samples
    for s in range(samples):
        chosen = inside & (group == groups[s].astype(F32))
        mean = jnp.sum(jnp.where(chosen, every, 0.0), keepdims=True) / GSIZE
        meansq = jnp.sum(jnp.where(chosen, every * every, 0.0), keepdims=True) / GSIZE
        value = (rewards[s] - mean) / jnp.sqrt(meansq - mean * mean + 0.25)
        advantage[s] = jnp.sum(value)
        log_prob[s] = jnp.sum(jnp.where(lane == s, logs, 0.0))
    each(lambda c: c.wait())


def local(
    frames,
    owners,
    offsets,
    groups,
    latent,
    noise_blocks,
    rewards,
    embed_weight,
    norm_gain,
    mid_weight,
    head_weight,
):
    samples = frames.shape[0]
    slots, channels, width = latent.shape
    maxb = slots // samples
    peers = lax.axis_size("dp")
    mp = lax.axis_size("mp")
    features, hidden = mid_weight.shape
    pair_cap = (slots + peers - 1) // peers
    per_pair = (pair_cap + mp - 1) // mp
    total = peers * per_pair
    share = (slots + 2 * mp - 1) // (2 * mp)
    owner_rows = 3 * samples
    tall = mp * hidden + 3 * channels
    params = functools.partial(pltpu.CompilerParams, vmem_limit_bytes=48 * 1024 * 1024)
    step = next(n for n in (256, 128, hidden) if hidden % n == 0)

    combined, gram, send, block_x, block_n, picks = pl.pallas_call(
        functools.partial(start_kernel, maxb, per_pair, mp, step),
        in_specs=[HBM] * 11,
        out_specs=[VMEM] * 6,
        out_shape=[
            jax.ShapeDtypeStruct((2 * channels, hidden), BF16),
            jax.ShapeDtypeStruct((3 * channels, channels), BF16),
            pltpu.VMEM((peers, per_pair * channels + META, width), BF16),
            jax.ShapeDtypeStruct((share, channels, 2 * width), BF16),
            jax.ShapeDtypeStruct((share, channels, 2 * width), BF16),
            jax.ShapeDtypeStruct((1, LANES), jnp.int32),
        ],
        scratch_shapes=[
            pltpu.SMEM((samples,), jnp.int32),
            pltpu.SMEM((slots,), jnp.int32),
            pltpu.SMEM((slots,), jnp.int32),
            pltpu.SMEM((samples,), jnp.int32),
            pltpu.SMEM((samples,), F32),
            pltpu.VMEM((channels, features), BF16),
            pltpu.VMEM((1, features), F32),
            pltpu.VMEM((features, hidden), BF16),
            pltpu.SMEM((peers,), jnp.int32),
            pltpu.SMEM((total,), jnp.int32),
            pltpu.SMEM((2 * share,), jnp.int32),
            pltpu.SemaphoreType.DMA((5,)),
            pltpu.SemaphoreType.DMA((3,)),
            pltpu.SemaphoreType.DMA((hidden // step,)),
            pltpu.SemaphoreType.DMA((total,)),
            pltpu.SemaphoreType.DMA((2 * share,)),
            pltpu.SemaphoreType.DMA((2 * share,)),
        ],
        compiler_params=params(),
        name="start",
    )(
        *map(
            in_hbm,
            (
                frames,
                owners,
                offsets,
                groups,
                rewards,
                latent,
                noise_blocks,
                embed_weight,
                norm_gain.reshape(1, features),
                mid_weight,
                head_weight.T,
            ),
        )
    )

    paired = mp & (mp - 1) == 0
    heads = [combined]
    for s in range(mp - 1, 0, -1):
        route = [(j, j ^ s if paired else (j + s) % mp) for j in range(mp)]
        heads.append(lax.ppermute(combined, "mp", route))
    recv = lax.all_to_all(send, "dp", split_axis=0, concat_axis=0, tiled=True)

    rows8 = (samples + 7) // 8 * 8
    errs, mt = pl.pallas_call(
        functools.partial(errors_kernel, mp, features),
        in_specs=[VMEM] * (4 + mp),
        out_specs=[VMEM, VMEM],
        out_shape=[
            jax.ShapeDtypeStruct((1, LANES), F32),
            jax.ShapeDtypeStruct((tall, channels), BF16),
        ],
        scratch_shapes=[
            pltpu.VMEM((rows8, width), F32),
            pltpu.SMEM((1, LANES), jnp.int32),
            pltpu.SemaphoreType.DMA,
        ],
        compiler_params=params(),
        name="errors",
    )(picks, block_x, block_n, gram, *heads)

    tail = (peers + META - 1) // META * META + META
    payload = pl.pallas_call(
        functools.partial(owner_kernel, per_pair, mp, features),
        in_specs=[VMEM] * (3 + mp),
        out_specs=VMEM,
        out_shape=jax.ShapeDtypeStruct((total * channels + tail, width), BF16),
        scratch_shapes=[pltpu.SMEM((total,), jnp.int32)],
        compiler_params=params(),
        name="owner",
    )(recv, errs, mt, *heads)

    gathered = lax.all_gather(payload, "mp", axis=0, tiled=False)

    return pl.pallas_call(
        functools.partial(place_kernel, per_pair),
        in_specs=[HBM] * 3 + [VMEM, VMEM],
        out_specs=[ANY, SMEM, SMEM],
        out_shape=[
            jax.ShapeDtypeStruct((owner_rows, channels, width), BF16),
            jax.ShapeDtypeStruct((samples,), F32),
            jax.ShapeDtypeStruct((samples,), F32),
        ],
        scratch_shapes=[
            pltpu.SMEM((samples,), jnp.int32),
            pltpu.SMEM((samples,), jnp.int32),
            pltpu.SMEM((samples,), F32),
            pltpu.VMEM((mp * peers, LANES), jnp.int32),
            pltpu.SMEM((mp * peers, LANES), jnp.int32),
            pltpu.SemaphoreType.DMA((3,)),
            pltpu.SemaphoreType.DMA((mp * total,)),
            pltpu.SemaphoreType.DMA,
        ],
        compiler_params=params(),
        name="place",
    )(in_hbm(frames), in_hbm(groups), in_hbm(rewards), recv, gathered)


def solution(mesh):
    placed = (
        P("dp"),
        P("dp"),
        P("dp"),
        P("dp"),
        P("dp", None, None),
        P("dp", None, None),
        P("dp"),
        P(),
        P(),
        P(None, "mp"),
        P("mp", None),
    )
    return jax.shard_map(
        local,
        mesh=mesh,
        in_specs=placed,
        out_specs=(P("dp", None, None), P("dp"), P("dp")),
        check_vma=False,
    )
```

```python
import functools

import jax
import jax.numpy as jnp
from jax import lax
from jax.experimental import pallas as pl
from jax.experimental.pallas import tpu as pltpu
from jax.sharding import PartitionSpec as P

GSIZE = 12
META = 16
LANES = 128
F32 = jnp.float32
BF16 = jnp.bfloat16
SMEM = pl.BlockSpec(memory_space=pltpu.SMEM)
VMEM = pl.BlockSpec(memory_space=pltpu.VMEM)
ANY = pl.BlockSpec(memory_space=pl.ANY)
HBM = pl.BlockSpec(memory_space=pltpu.HBM)


def in_hbm(value):
    return pltpu.with_memory_space_constraint(value, pltpu.HBM)


def split3(value):
    hi = value.astype(BF16)
    rest = value - hi.astype(F32)
    mid = rest.astype(BF16)
    lo = (rest - mid.astype(F32)).astype(BF16)
    return hi, mid, lo


def lane_row(scalars, count, dtype):
    lane = lax.broadcasted_iota(jnp.int32, (1, LANES), 1)
    row = jnp.zeros((1, LANES), dtype)
    for s in range(count):
        row = jnp.where(lane == s, scalars(s), row)
    return row


def live_count(frames, sample):
    return lax.shift_right_logical(frames[sample] - 1, 5) + 1


def rest_of(value, mp):
    return lax.bitwise_and(value, mp - 1) if mp & (mp - 1) == 0 else lax.rem(value, mp)


def part_of(value, mp):
    return lax.shift_right_logical(value, mp.bit_length() - 1) if mp & (mp - 1) == 0 else value // mp


def start_kernel(
    maxb,
    per_pair,
    mp,
    step,
    frames_h,
    owners_h,
    offsets_h,
    groups_h,
    rewards_h,
    latent,
    noise,
    embed_h,
    gain_h,
    weight,
    head_h,
    out,
    gram,
    send,
    block_x,
    block_n,
    picks,
    frames,
    owners,
    offsets,
    groups,
    rewards,
    embed,
    gain,
    held,
    places,
    rows,
    source,
    chosen,
    slot_of,
    small_sems,
    big_sems,
    weight_sems,
    row_sems,
    x_sems,
    n_sems,
):
    peers = send.shape[0]
    _, channels, width = latent.shape
    hidden = weight.shape[1]
    samples = frames.shape[0]
    share = block_x.shape[0] * 2
    total = peers * per_pair
    small = [
        pltpu.make_async_copy(a, b, small_sems.at[n])
        for n, (a, b) in enumerate(
            [
                (frames_h, frames),
                (owners_h, owners),
                (offsets_h, offsets),
                (groups_h, groups),
                (rewards_h, rewards),
            ]
        )
    ]
    big = [
        pltpu.make_async_copy(embed_h, embed, big_sems.at[0]),
        pltpu.make_async_copy(gain_h, gain, big_sems.at[1]),
        pltpu.make_async_copy(head_h, out.at[pl.ds(channels, channels)], big_sems.at[2]),
    ]
    parts = [
        pltpu.make_async_copy(weight.at[:, pl.ds(n, step)], held.at[:, pl.ds(n, step)], weight_sems.at[n // step])
        for n in range(0, hidden, step)
    ]
    for copy in small + big[:2] + parts + big[2:]:
        copy.start()

    me = lax.axis_index("mp")
    shift = rest_of(me + mp - rest_of(lax.axis_index("dp"), mp), mp)
    for o in range(peers + 1):
        places[o] = 0
    for n in range(total + 1):
        rows[n] = 0
        source[n] = 0
    for j in range(share + 1):
        chosen[j] = 0
        slot_of[j] = 0
    for copy in small:
        copy.wait()
    seen = jnp.int32(0)
    count = jnp.int32(0)
    for s in range(samples):
        live_here = live_count(frames, s)
        for k in range(maxb):
            i = s * maxb + k
            live = k < live_here
            o = jnp.where(live, owners[i], peers)
            place = places[o]
            places[o] = place + 1
            q = part_of(place, mp)
            sends = live & (rest_of(place, mp) == shift) & (q < per_pair)
            n = jnp.where(sends, o * per_pair + q, total)
            rows[n] = offsets[i] + 1
            source[n] = i
            chosen[count] = s
            slot_of[count] = i
            mine = live & (rest_of(seen, mp) == me)
            seen = seen + live.astype(jnp.int32)
            count = count + mine.astype(jnp.int32)

    copies = [
        pltpu.make_async_copy(
            latent.at[source[o * per_pair + q]],
            send.at[o, pl.ds(q * channels, channels)],
            row_sems.at[o * per_pair + q],
        )
        for o in range(peers)
        for q in range(per_pair)
    ]
    for j in range(share):
        lanes = pl.ds(j % 2 * width, width)
        copies.append(pltpu.make_async_copy(latent.at[slot_of[j]], block_x.at[j // 2, :, lanes], x_sems.at[j]))
        copies.append(pltpu.make_async_copy(noise.at[slot_of[j]], block_n.at[j // 2, :, lanes], n_sems.at[j]))
    for copy in copies:
        copy.start()

    lane = lax.broadcasted_iota(jnp.int32, (1, LANES), 1)
    found = jnp.where(lane == LANES - 1, count, 0)
    for j in range(share):
        found = jnp.where(lane == j, chosen[j], found)
    picks[...] = found

    hi, mid, lo = split3(lane_row(lambda s: rewards[s], samples, F32))
    group = lane_row(lambda s: groups[s].astype(F32), samples, F32)
    sub = lax.broadcasted_iota(jnp.int32, (META, LANES), 0)
    shared = jnp.where(sub == 1, hi.astype(F32), 0.0)
    shared = jnp.where(sub == 2, mid.astype(F32), shared)
    shared = jnp.where(sub == 3, lo.astype(F32), shared)
    shared = jnp.where(sub == 4, group, shared)
    for o in range(peers):
        first = lane_row(lambda q: rows[o * per_pair + q].astype(F32), per_pair, F32)
        send[o, pl.ds(per_pair * channels, META), :] = jnp.where(sub == 0, first, shared).astype(BF16)

    big[0].wait()
    e = embed[...]
    big[1].wait()
    scaled = e.astype(F32) * gain[...]
    hi = scaled.astype(BF16)
    lo = (scaled - hi.astype(F32)).astype(BF16)
    both = jnp.concatenate([hi, lo], axis=0)
    for n, copy in enumerate(parts):
        copy.wait()
        m = jnp.dot(both, held[:, n * step : (n + 1) * step], preferred_element_type=F32)
        out[:channels, n * step : (n + 1) * step] = (m[:channels] + m[channels:]).astype(BF16)
    hi, mid, lo = split3(lax.dot_general(e, e, (((1,), (1,)), ((), ())), preferred_element_type=F32))
    gram[...] = jnp.concatenate([hi, mid, lo], axis=0)
    big[2].wait()
    for copy in copies:
        copy.wait()


def norm_factor(x, gram, features):
    channels = x.shape[0]
    g = jnp.dot(gram, x, preferred_element_type=F32)
    gx = g[:channels] + g[channels : 2 * channels] + g[2 * channels :]
    mean_sq = jnp.sum(gx * x.astype(F32), axis=0, keepdims=True) * (1.0 / features)
    return 0.5 * lax.rsqrt(jnp.maximum(mean_sq, 0.0) + 0.25)


def velocity(x, half, mt, heads, total=None):
    channels, hidden = heads[0].shape[0] // 2, heads[0].shape[1]
    for m, head in enumerate(heads):
        mid = jnp.dot(mt[m * hidden : (m + 1) * hidden, :], x, preferred_element_type=F32)
        v = mid * half
        act = (v + v * jnp.tanh(v)).astype(BF16)
        part = jnp.dot(head[channels:, :], act, preferred_element_type=F32)
        total = part if total is None else total + part
    return total


def turn(mt, heads):
    channels, hidden = heads[0].shape[0] // 2, heads[0].shape[1]
    for m, head in enumerate(heads):
        mt[m * hidden : (m + 1) * hidden, :] = head[:channels, :].T


def early_kernel(near, features, picks, block_x, gram, *refs):
    heads, (partial, halves, mt, table, sem) = refs[:near], refs[near:]
    copy = pltpu.make_async_copy(picks, table, sem)
    copy.start()
    turn(mt, heads)
    copy.wait()
    count = table[0, LANES - 1]

    def body(pair, carry):
        x = block_x[pair]
        half = norm_factor(x, gram[...], features)
        halves[pair] = half
        partial[pair] = velocity(x, half, mt, heads)
        return carry

    lax.fori_loop(0, (count + 1) // 2, body, 0)


def errors_kernel(far, picks, block_x, block_n, partial, halves, *refs):
    heads, (errs, mt, acc, table, sem) = refs[:far], refs[far:]
    width = block_x.shape[2] // 2
    copy = pltpu.make_async_copy(picks, table, sem)
    copy.start()
    turn(mt, heads)
    acc[...] = jnp.zeros_like(acc)
    copy.wait()
    count = table[0, LANES - 1]

    def body(pair, carry):
        v = velocity(block_x[pair], halves[pair], mt, heads, partial[pair])
        e = block_n[pair].astype(F32) + v
        rows = jnp.sum(e * e, axis=0, keepdims=True)
        acc[pl.ds(table[0, 2 * pair], 1), :] += rows[:, :width]

        @pl.when(2 * pair + 1 < count)
        def _():
            acc[pl.ds(table[0, 2 * pair + 1], 1), :] += rows[:, width:]

        return carry

    lax.fori_loop(0, (count + 1) // 2, body, 0)
    sums = jnp.sum(acc[...], axis=1, keepdims=True)
    lane = lax.broadcasted_iota(jnp.int32, acc.shape, 1)
    sub = lax.broadcasted_iota(jnp.int32, acc.shape, 0)
    errs[...] = jnp.sum(jnp.where(lane == sub, sums, 0.0), axis=0, keepdims=True)


def owner_kernel(per_pair, near, shards, features, recv, errs, gram, mt_near, mt_far, *refs):
    heads, (out, order) = refs[:shards], refs[shards:]
    peers = recv.shape[0]
    channels = heads[0].shape[0] // 2
    total = peers * per_pair
    base = total * channels
    first = recv[:, per_pair * channels, :].astype(F32)
    out[base : base + peers, :] = first.astype(BF16)
    hi, mid, lo = split3(errs[...])
    sub = lax.broadcasted_iota(jnp.int32, (META, LANES), 0)
    meta = jnp.where(sub == 0, hi.astype(F32), 0.0)
    meta = jnp.where(sub == 1, mid.astype(F32), meta)
    meta = jnp.where(sub == 2, lo.astype(F32), meta)
    out[out.shape[0] - META :, :] = meta.astype(BF16)
    lane = lax.broadcasted_iota(jnp.int32, (peers, LANES), 1)
    number = lax.broadcasted_iota(jnp.int32, (peers, LANES), 0) * per_pair + lane
    count = jnp.int32(0)
    for low in range(0, total, 16):
        inside = (lane < per_pair) & (number >= low) & (number < low + 16) & (first > 0)
        bits = jnp.where(inside, lax.shift_left(1, jnp.clip(number - low, 0, 15)).astype(F32), 0.0)
        mask = jnp.sum(bits).astype(jnp.int32)
        for n in range(low, min(low + 16, total)):
            order[count] = n
            count = count + lax.bitwise_and(lax.shift_right_logical(mask, n - low), 1)

    def body(pair, carry):
        one = order[2 * pair]
        more = 2 * pair + 1 < count
        two = jnp.where(more, order[2 * pair + 1], one)
        x = jnp.concatenate(
            [
                recv[n // per_pair, pl.ds(pl.multiple_of((n % per_pair) * channels, channels), channels), :]
                for n in (one, two)
            ],
            axis=1,
        )
        half = norm_factor(x, gram[...], features)
        v = velocity(x, half, mt_near, heads[:near])
        v = velocity(x, half, mt_far, heads[near:], v).astype(BF16)
        width = v.shape[1] // 2
        out[pl.ds(pl.multiple_of(one * channels, channels), channels), :] = v[:, :width]

        @pl.when(more)
        def _():
            out[pl.ds(pl.multiple_of(two * channels, channels), channels), :] = v[:, width:]

        return carry

    lax.fori_loop(0, (count + 1) // 2, body, 0)


def place_kernel(
    per_pair,
    frames_h,
    groups_h,
    rewards_h,
    recv,
    gathered,
    pred,
    log_out,
    adv_out,
    frames,
    groups,
    rewards,
    log_prob,
    advantage,
    small_sems,
    sem,
):
    shards = gathered.shape[0]
    rows_here, channels, width = pred.shape
    peers = recv.shape[0]
    total = peers * per_pair
    samples = frames.shape[0]
    base = total * channels
    small = [
        pltpu.make_async_copy(a, b, small_sems.at[n])
        for n, (a, b) in enumerate([(frames_h, frames), (groups_h, groups), (rewards_h, rewards)])
    ]
    for copy in small:
        copy.start()
    bits = rows_here.bit_length()
    pack = 24 // bits
    lane8 = lax.broadcasted_iota(jnp.int32, (peers, LANES), 1)
    number = lax.broadcasted_iota(jnp.int32, (peers, LANES), 0) * per_pair + lane8
    scale = lax.shift_left(1, bits * lax.rem(number, pack)).astype(F32)
    for m in range(shards):
        first = gathered[m, base : base + peers, :].astype(F32)
        for low in range(0, total, pack):
            inside = (lane8 < per_pair) & (number >= low) & (number < low + pack)
            code = jnp.sum(jnp.where(inside, first * scale, 0.0)).astype(jnp.int32)
            for n in range(low, min(low + pack, total)):
                row = lax.bitwise_and(lax.shift_right_logical(code, bits * (n - low)), 2**bits - 1)

                @pl.when(row > 0)
                def _():
                    pltpu.make_async_copy(
                        gathered.at[m, pl.ds(n * channels, channels)], pred.at[row - 1], sem
                    ).start()

    for copy in small:
        copy.wait()
    lane = lax.broadcasted_iota(jnp.int32, (1, LANES), 1)
    sums = jnp.zeros((1, LANES), F32)
    for m in range(shards):
        part = gathered[m, gathered.shape[1] - META :, :].astype(F32)
        sums = sums + (part[0:1] + part[1:2] + part[2:3])
    size = lane_row(lambda s: (live_count(frames, s) * (channels * width)).astype(F32), samples, F32)
    logs = -0.5 * sums / jnp.where(lane < samples, size, 1.0)

    info = recv[:, pl.ds(per_pair * channels, META), :].astype(F32)
    every = info[:, 1, :] + info[:, 2, :] + info[:, 3, :]
    group = info[:, 4, :]
    inside = lax.broadcasted_iota(jnp.int32, every.shape, 1) < samples
    for s in range(samples):
        chosen = inside & (group == groups[s].astype(F32))
        mean = jnp.sum(jnp.where(chosen, every, 0.0), keepdims=True) / GSIZE
        meansq = jnp.sum(jnp.where(chosen, every * every, 0.0), keepdims=True) / GSIZE
        value = (rewards[s] - mean) / jnp.sqrt(meansq - mean * mean + 0.25)
        advantage[s] = jnp.sum(value)
        log_prob[s] = jnp.sum(jnp.where(lane == s, logs, 0.0))
    last = [
        pltpu.make_async_copy(log_prob, log_out, small_sems.at[0]),
        pltpu.make_async_copy(advantage, adv_out, small_sems.at[1]),
    ]
    for copy in last:
        copy.start()
    pltpu.make_async_copy(pred, pred, sem).wait()
    for copy in last:
        copy.wait()


def local(
    frames,
    owners,
    offsets,
    groups,
    latent,
    noise_blocks,
    rewards,
    embed_weight,
    norm_gain,
    mid_weight,
    head_weight,
):
    samples = frames.shape[0]
    slots, channels, width = latent.shape
    maxb = slots // samples
    peers = lax.axis_size("dp")
    mp = lax.axis_size("mp")
    features, hidden = mid_weight.shape
    pair_cap = (slots + peers - 1) // peers
    per_pair = (pair_cap + mp - 1) // mp
    total = peers * per_pair
    share = (slots + 2 * mp - 1) // (2 * mp)
    owner_rows = 3 * samples
    params = functools.partial(pltpu.CompilerParams, vmem_limit_bytes=48 * 1024 * 1024)
    step = next(n for n in (256, 128, hidden) if hidden % n == 0)

    combined, gram, send, block_x, block_n, picks = pl.pallas_call(
        functools.partial(start_kernel, maxb, per_pair, mp, step),
        in_specs=[HBM] * 11,
        out_specs=[VMEM] * 6,
        out_shape=[
            jax.ShapeDtypeStruct((2 * channels, hidden), BF16),
            jax.ShapeDtypeStruct((3 * channels, channels), BF16),
            pltpu.VMEM((peers, per_pair * channels + META, width), BF16),
            jax.ShapeDtypeStruct((share, channels, 2 * width), BF16),
            jax.ShapeDtypeStruct((share, channels, 2 * width), BF16),
            jax.ShapeDtypeStruct((1, LANES), jnp.int32),
        ],
        scratch_shapes=[
            pltpu.SMEM((samples,), jnp.int32),
            pltpu.SMEM((slots,), jnp.int32),
            pltpu.SMEM((slots,), jnp.int32),
            pltpu.SMEM((samples,), jnp.int32),
            pltpu.SMEM((samples,), F32),
            pltpu.VMEM((channels, features), BF16),
            pltpu.VMEM((1, features), F32),
            pltpu.VMEM((features, hidden), BF16),
            pltpu.SMEM((peers + 1,), jnp.int32),
            pltpu.SMEM((total + 1,), jnp.int32),
            pltpu.SMEM((total + 1,), jnp.int32),
            pltpu.SMEM((2 * share + 1,), jnp.int32),
            pltpu.SMEM((2 * share + 1,), jnp.int32),
            pltpu.SemaphoreType.DMA((5,)),
            pltpu.SemaphoreType.DMA((3,)),
            pltpu.SemaphoreType.DMA((hidden // step,)),
            pltpu.SemaphoreType.DMA((total,)),
            pltpu.SemaphoreType.DMA((2 * share,)),
            pltpu.SemaphoreType.DMA((2 * share,)),
        ],
        compiler_params=params(),
        name="start",
    )(
        *map(
            in_hbm,
            (
                frames,
                owners,
                offsets,
                groups,
                rewards,
                latent,
                noise_blocks,
                embed_weight,
                norm_gain.reshape(1, features),
                mid_weight,
                head_weight.T,
            ),
        )
    )

    paired = mp & (mp - 1) == 0
    near = max(mp // 2, 1)
    heads = [combined]
    for s in range(1, mp):
        route = [(j, j ^ s if paired else (j + s) % mp) for j in range(mp)]
        heads.append(lax.ppermute(combined, "mp", route))
    recv = lax.all_to_all(send, "dp", split_axis=0, concat_axis=0, tiled=True)

    partial, halves, mt_near = pl.pallas_call(
        functools.partial(early_kernel, near, features),
        in_specs=[VMEM] * (3 + near),
        out_specs=[VMEM] * 3,
        out_shape=[
            jax.ShapeDtypeStruct((share, channels, 2 * width), F32),
            jax.ShapeDtypeStruct((share, 1, 2 * width), F32),
            jax.ShapeDtypeStruct((near * hidden, channels), BF16),
        ],
        scratch_shapes=[pltpu.SMEM((1, LANES), jnp.int32), pltpu.SemaphoreType.DMA],
        compiler_params=params(),
        name="early",
    )(picks, block_x, gram, *heads[:near])

    rows8 = (samples + 7) // 8 * 8
    errs, mt_far = pl.pallas_call(
        functools.partial(errors_kernel, mp - near),
        in_specs=[VMEM] * (5 + mp - near),
        out_specs=[VMEM, VMEM],
        out_shape=[
            jax.ShapeDtypeStruct((1, LANES), F32),
            jax.ShapeDtypeStruct(((mp - near) * hidden, channels), BF16),
        ],
        scratch_shapes=[
            pltpu.VMEM((rows8, width), F32),
            pltpu.SMEM((1, LANES), jnp.int32),
            pltpu.SemaphoreType.DMA,
        ],
        compiler_params=params(),
        name="errors",
    )(picks, block_x, block_n, partial, halves, *heads[near:])

    tail = (peers + META - 1) // META * META + META
    payload = pl.pallas_call(
        functools.partial(owner_kernel, per_pair, near, mp, features),
        in_specs=[VMEM] * (5 + mp),
        out_specs=VMEM,
        out_shape=jax.ShapeDtypeStruct((total * channels + tail, width), BF16),
        scratch_shapes=[pltpu.SMEM((total + 1,), jnp.int32)],
        compiler_params=params(),
        name="owner",
    )(recv, errs, gram, mt_near, mt_far, *heads)

    gathered = lax.all_gather(payload, "mp", axis=0, tiled=False)

    return pl.pallas_call(
        functools.partial(place_kernel, per_pair),
        in_specs=[HBM] * 3 + [VMEM, VMEM],
        out_specs=[ANY] * 3,
        out_shape=[
            jax.ShapeDtypeStruct((owner_rows, channels, width), BF16),
            jax.ShapeDtypeStruct((samples,), F32),
            jax.ShapeDtypeStruct((samples,), F32),
        ],
        scratch_shapes=[
            pltpu.SMEM((samples,), jnp.int32),
            pltpu.SMEM((samples,), jnp.int32),
            pltpu.SMEM((samples,), F32),
            pltpu.SMEM((samples,), F32),
            pltpu.SMEM((samples,), F32),
            pltpu.SemaphoreType.DMA((3,)),
            pltpu.SemaphoreType.DMA,
        ],
        compiler_params=params(),
        name="place",
    )(in_hbm(frames), in_hbm(groups), in_hbm(rewards), recv, gathered)


def solution(mesh):
    placed = (
        P("dp"),
        P("dp"),
        P("dp"),
        P("dp"),
        P("dp", None, None),
        P("dp", None, None),
        P("dp"),
        P(),
        P(),
        P(None, "mp"),
        P("mp", None),
    )
    return jax.shard_map(
        local,
        mesh=mesh,
        in_specs=placed,
        out_specs=(P("dp", None, None), P("dp"), P("dp")),
        check_vma=False,
    )
```

```python
import functools

import jax
import jax.numpy as jnp
from jax import lax
from jax.experimental import pallas as pl
from jax.experimental.pallas import tpu as pltpu
from jax.sharding import PartitionSpec as P

GSIZE = 12
META = 8
LANES = 128
F32 = jnp.float32
BF16 = jnp.bfloat16
SMEM = pl.BlockSpec(memory_space=pltpu.SMEM)
VMEM = pl.BlockSpec(memory_space=pltpu.VMEM)
ANY = pl.BlockSpec(memory_space=pl.ANY)
HBM = pl.BlockSpec(memory_space=pltpu.HBM)


def in_hbm(value):
    return pltpu.with_memory_space_constraint(value, pltpu.HBM)


def split3(value):
    hi = value.astype(BF16)
    rest = value - hi.astype(F32)
    mid = rest.astype(BF16)
    lo = (rest - mid.astype(F32)).astype(BF16)
    return hi, mid, lo


def lane_row(scalars, count, dtype):
    lane = lax.broadcasted_iota(jnp.int32, (1, LANES), 1)
    row = jnp.zeros((1, LANES), dtype)
    for s in range(count):
        row = jnp.where(lane == s, scalars(s), row)
    return row


def live_count(frames, sample):
    return lax.shift_right_logical(frames[sample] - 1, 5) + 1


def rest_of(value, mp):
    return lax.bitwise_and(value, mp - 1) if mp & (mp - 1) == 0 else lax.rem(value, mp)


def part_of(value, mp):
    return lax.shift_right_logical(value, mp.bit_length() - 1) if mp & (mp - 1) == 0 else value // mp


def start_kernel(
    maxb,
    per_pair,
    mp,
    step,
    frames_h,
    owners_h,
    offsets_h,
    groups_h,
    rewards_h,
    latent,
    noise,
    embed_h,
    gain_h,
    weight,
    head_h,
    out,
    gram,
    send,
    block_x,
    block_n,
    picks,
    info,
    frames,
    owners,
    offsets,
    groups,
    rewards,
    embed,
    gain,
    held,
    packed,
    places,
    rows,
    source,
    chosen,
    slot_of,
    small_sems,
    big_sems,
    weight_sems,
    row_sems,
    x_sems,
    n_sems,
    leave_sem,
):
    peers = send.shape[0]
    _, channels, width = latent.shape
    hidden = weight.shape[1]
    samples = frames.shape[0]
    share = block_x.shape[0] * 2
    total = peers * per_pair
    small = [
        pltpu.make_async_copy(a, b, small_sems.at[n])
        for n, (a, b) in enumerate(
            [
                (frames_h, frames),
                (owners_h, owners),
                (offsets_h, offsets),
                (groups_h, groups),
                (rewards_h, rewards),
            ]
        )
    ]
    big = [
        pltpu.make_async_copy(embed_h, embed, big_sems.at[0]),
        pltpu.make_async_copy(gain_h, gain, big_sems.at[1]),
        pltpu.make_async_copy(head_h, out.at[pl.ds(channels, channels)], big_sems.at[2]),
    ]
    parts = [
        pltpu.make_async_copy(weight.at[:, pl.ds(n, step)], held.at[:, pl.ds(n, step)], weight_sems.at[n // step])
        for n in range(0, hidden, step)
    ]
    for copy in small + big[:2] + parts + big[2:]:
        copy.start()

    me = lax.axis_index("mp")
    shift = rest_of(me + mp - rest_of(lax.axis_index("dp"), mp), mp)
    for o in range(peers + 1):
        places[o] = 0
    for n in range(total + 1):
        rows[n] = 0
        source[n] = 0
    for j in range(share + 1):
        chosen[j] = 0
        slot_of[j] = 0
    for copy in small:
        copy.wait()
    seen = jnp.int32(0)
    count = jnp.int32(0)
    for s in range(samples):
        live_here = live_count(frames, s)
        for k in range(maxb):
            i = s * maxb + k
            live = k < live_here
            o = jnp.where(live, owners[i], peers)
            place = places[o]
            places[o] = place + 1
            q = part_of(place, mp)
            sends = live & (rest_of(place, mp) == shift) & (q < per_pair)
            n = jnp.where(sends, o * per_pair + q, total)
            rows[n] = offsets[i] + 1
            source[n] = i
            chosen[count] = s
            slot_of[count] = i
            mine = live & (rest_of(seen, mp) == me)
            seen = seen + live.astype(jnp.int32)
            count = count + mine.astype(jnp.int32)

    copies = [
        pltpu.make_async_copy(
            latent.at[source[o * per_pair + q]],
            packed.at[o, pl.ds(q * channels, channels)],
            row_sems.at[o * per_pair + q],
        )
        for o in range(peers)
        for q in range(per_pair)
    ]
    for j in range(share):
        lanes = pl.ds(j % 2 * width, width)
        copies.append(pltpu.make_async_copy(latent.at[slot_of[j]], block_x.at[j // 2, :, lanes], x_sems.at[j]))
        copies.append(pltpu.make_async_copy(noise.at[slot_of[j]], block_n.at[j // 2, :, lanes], n_sems.at[j]))
    for copy in copies:
        copy.start()
    leave = pltpu.make_async_copy(packed, send, leave_sem)

    sub = lax.broadcasted_iota(jnp.int32, picks.shape, 0)
    found = jnp.full(picks.shape, -1, jnp.int32)
    for j in range(share):
        found = jnp.where((sub == j) & (j < count), chosen[j], found)
    picks[...] = found

    reward = lane_row(lambda s: rewards[s], samples, F32)
    group = lane_row(lambda s: groups[s].astype(F32), samples, F32)
    counts = lane_row(lambda s: live_count(frames, s).astype(F32), samples, F32)
    hi, mid, lo = split3(reward)
    sub = lax.broadcasted_iota(jnp.int32, (META, LANES), 0)
    info[...] = jnp.where(sub == 0, reward, jnp.where(sub == 1, group, counts))
    shared = jnp.where(sub == 1, hi.astype(F32), 0.0)
    shared = jnp.where(sub == 2, mid.astype(F32), shared)
    shared = jnp.where(sub == 3, lo.astype(F32), shared)
    shared = jnp.where(sub == 4, group, shared)
    for o in range(peers):
        first = lane_row(lambda q: rows[o * per_pair + q].astype(F32), per_pair, F32)
        packed[o, pl.ds(per_pair * channels, META), :] = jnp.where(sub == 0, first, shared).astype(BF16)

    big[0].wait()
    e = embed[...]
    big[1].wait()
    scaled = e.astype(F32) * gain[...]
    hi = scaled.astype(BF16)
    lo = (scaled - hi.astype(F32)).astype(BF16)
    both = jnp.concatenate([hi, lo], axis=0)
    for n, copy in enumerate(parts):
        copy.wait()
        m = jnp.dot(both, held[:, n * step : (n + 1) * step], preferred_element_type=F32)
        out[:channels, n * step : (n + 1) * step] = (m[:channels] + m[channels:]).astype(BF16)
        if n == 0:
            for one in copies[:total]:
                one.wait()
            leave.start()
    hi, mid, lo = split3(lax.dot_general(e, e, (((1,), (1,)), ((), ())), preferred_element_type=F32))
    gram[...] = jnp.concatenate([hi, mid, lo], axis=0)
    big[2].wait()
    for copy in copies[total:]:
        copy.wait()
    leave.wait()


def norm_factors(xs, gram, features):
    channels, width = xs[0].shape
    x = jnp.concatenate(xs, axis=1)
    g = jnp.dot(gram, x, preferred_element_type=F32)
    gx = g[:channels] + g[channels : 2 * channels] + g[2 * channels :]
    mean_sq = jnp.sum(gx * x.astype(F32), axis=0, keepdims=True) * (1.0 / features)
    half = 0.5 * lax.rsqrt(jnp.maximum(mean_sq, 0.0) + 0.25)
    return [half[:, p * width : (p + 1) * width] for p in range(len(xs))]


def velocities(xs, halves, parts, totals):
    totals = list(totals)
    waiting = []

    def finish():
        p, head, act = waiting.pop()
        part = jnp.dot(head, act, preferred_element_type=F32)
        totals[p] = part if totals[p] is None else totals[p] + part

    for p, x in enumerate(xs):
        for mt, both, row in parts:
            channels, hidden = both.shape[0] // 2, both.shape[1]
            mid = jnp.dot(mt[row : row + hidden, :], x, preferred_element_type=F32)
            if waiting:
                finish()
            v = mid * halves[p]
            waiting.append((p, both[channels:, :], (v + v * jnp.tanh(v)).astype(BF16)))
    finish()
    return totals


def turn(mt, heads):
    channels, hidden = heads[0].shape[0] // 2, heads[0].shape[1]
    for m, head in enumerate(heads):
        mt[m * hidden : (m + 1) * hidden, :] = head[:channels, :].T


def shards_of(mt, heads):
    hidden = heads[0].shape[1]
    return [(mt, head, m * hidden) for m, head in enumerate(heads)]


def early_kernel(near, features, block_x, gram, *refs):
    heads, (partial, halves, mt) = refs[:near], refs[near:]
    turn(mt, heads)
    xs = [block_x[p] for p in range(block_x.shape[0])]
    half = norm_factors(xs, gram[...], features)
    for p, total in enumerate(velocities(xs, half, shards_of(mt, heads), [None] * len(xs))):
        halves[p] = half[p]
        partial[p] = total


def errors_kernel(far, picks, block_x, block_n, partial, halves, *refs):
    heads, (errs, mt) = refs[:far], refs[far:]
    pairs, _, double = block_x.shape
    width = double // 2
    turn(mt, heads)
    xs = [block_x[p] for p in range(pairs)]
    half = [halves[p] for p in range(pairs)]
    totals = velocities(xs, half, shards_of(mt, heads), [partial[p] for p in range(pairs)])
    sub = lax.broadcasted_iota(jnp.int32, picks.shape, 0)
    lane = lax.broadcasted_iota(jnp.int32, picks.shape, 1)
    sums = jnp.zeros(picks.shape, F32)
    for p, v in enumerate(totals):
        e = block_n[p].astype(F32) + v
        line = jnp.sum(e * e, axis=0, keepdims=True)
        sums = jnp.where(sub == 2 * p, line[:, :width], sums)
        sums = jnp.where(sub == 2 * p + 1, line[:, width:], sums)
    each = jnp.sum(sums, axis=1, keepdims=True)
    errs[...] = jnp.sum(jnp.where(lane == picks[...], each, 0.0), axis=0, keepdims=True)


def owner_kernel(per_pair, near, shards, features, recv, errs, gram, mt_near, mt_far, *refs):
    heads, (out, order) = refs[:shards], refs[shards:]
    peers = recv.shape[0]
    channels = heads[0].shape[0] // 2
    total = peers * per_pair
    base = total * channels
    first = recv[:, per_pair * channels, :].astype(F32)
    out[base : base + peers, :] = first.astype(BF16)
    hi, mid, lo = split3(errs[...])
    sub = lax.broadcasted_iota(jnp.int32, (META, LANES), 0)
    meta = jnp.where(sub == 0, hi.astype(F32), 0.0)
    meta = jnp.where(sub == 1, mid.astype(F32), meta)
    meta = jnp.where(sub == 2, lo.astype(F32), meta)
    out[out.shape[0] - META :, :] = meta.astype(BF16)
    lane = lax.broadcasted_iota(jnp.int32, (peers, LANES), 1)
    number = lax.broadcasted_iota(jnp.int32, (peers, LANES), 0) * per_pair + lane
    count = jnp.int32(0)
    for low in range(0, total, 16):
        inside = (lane < per_pair) & (number >= low) & (number < low + 16) & (first > 0)
        bits = jnp.where(inside, lax.shift_left(1, jnp.clip(number - low, 0, 15)).astype(F32), 0.0)
        mask = jnp.sum(bits).astype(jnp.int32)
        for n in range(low, min(low + 16, total)):
            order[count] = n
            count = count + lax.bitwise_and(lax.shift_right_logical(mask, n - low), 1)
    parts = shards_of(mt_near, heads[:near]) + shards_of(mt_far, heads[near:])

    def block_of(n):
        if per_pair == 1:
            return recv[n, :channels, :]
        return recv[n // per_pair, pl.ds(pl.multiple_of((n % per_pair) * channels, channels), channels), :]

    def run(begin, pairs):
        slots = [order[jnp.minimum(begin + j, count - 1)] for j in range(2 * pairs)]
        xs = [
            jnp.concatenate([block_of(slots[2 * p]), block_of(slots[2 * p + 1])], axis=1)
            for p in range(pairs)
        ]
        half = norm_factors(xs, gram[...], features)
        for p, v in enumerate(velocities(xs, half, parts, [None] * pairs)):
            v = v.astype(BF16)
            width = v.shape[1] // 2
            for j in range(2):
                at = pl.multiple_of(slots[2 * p + j] * channels, channels)
                out[pl.ds(at, channels), :] = v[:, j * width : (j + 1) * width]

    def quad(n, carry):
        left = (jnp.clip(count - 8 * n, 0, 8) + 1) // 2
        for pairs in range(1, 5):

            @pl.when(left == pairs)
            def _():
                run(8 * n, pairs)

        return carry

    if total <= 8:
        quad(0, 0)
    else:
        lax.fori_loop(0, (total + 7) // 8, quad, 0)


def place_kernel(per_pair, samples, info, recv, gathered, pred, log_out, adv_out, log_prob, advantage, small_sems, sem):
    shards = gathered.shape[0]
    rows_here, channels, width = pred.shape
    peers = recv.shape[0]
    total = peers * per_pair
    base = total * channels
    bits = rows_here.bit_length()
    pack = 24 // bits
    lane8 = lax.broadcasted_iota(jnp.int32, (peers, LANES), 1)
    number = lax.broadcasted_iota(jnp.int32, (peers, LANES), 0) * per_pair + lane8
    scale = lax.shift_left(1, bits * lax.rem(number, pack)).astype(F32)
    for m in range(shards):
        first = gathered[m, base : base + peers, :].astype(F32)
        for low in range(0, total, pack):
            inside = (lane8 < per_pair) & (number >= low) & (number < low + pack)
            code = jnp.sum(jnp.where(inside, first * scale, 0.0)).astype(jnp.int32)
            for n in range(low, min(low + pack, total)):
                row = lax.bitwise_and(lax.shift_right_logical(code, bits * (n - low)), 2**bits - 1)

                @pl.when(row > 0)
                def _():
                    pltpu.make_async_copy(
                        gathered.at[m, pl.ds(n * channels, channels)], pred.at[row - 1], sem
                    ).start()

    lane = lax.broadcasted_iota(jnp.int32, (1, LANES), 1)
    sums = jnp.zeros((1, LANES), F32)
    for m in range(shards):
        part = gathered[m, gathered.shape[1] - META :, :].astype(F32)
        sums = sums + (part[0:1] + part[1:2] + part[2:3])
    reward, own_group, counts = info[0:1, :], info[1:2, :], info[2:3, :]
    size = jnp.where(lane < samples, counts * float(channels * width), 1.0)
    logs = -0.5 * sums / size

    meta = recv[:, pl.ds(per_pair * channels, META), :].astype(F32)
    every = meta[:, 1, :] + meta[:, 2, :] + meta[:, 3, :]
    group = jnp.where(lax.broadcasted_iota(jnp.int32, every.shape, 1) < samples, meta[:, 4, :], -1.0)
    mean = jnp.zeros((1, LANES), F32)
    meansq = jnp.zeros((1, LANES), F32)
    for s in range(samples):
        mine = jnp.sum(jnp.where(lane == s, own_group, 0.0), axis=1, keepdims=True)
        chosen = group == mine
        one = jnp.sum(jnp.sum(jnp.where(chosen, every, 0.0), axis=0, keepdims=True), axis=1, keepdims=True)
        two = jnp.sum(jnp.sum(jnp.where(chosen, every * every, 0.0), axis=0, keepdims=True), axis=1, keepdims=True)
        mean = jnp.where(lane == s, one / GSIZE, mean)
        meansq = jnp.where(lane == s, two / GSIZE, meansq)
    scores = (reward - mean) / jnp.sqrt(meansq - mean * mean + 0.25)
    for s in range(samples):
        advantage[s] = jnp.sum(jnp.where(lane == s, scores, 0.0))
        log_prob[s] = jnp.sum(jnp.where(lane == s, logs, 0.0))
    last = [
        pltpu.make_async_copy(log_prob, log_out, small_sems.at[0]),
        pltpu.make_async_copy(advantage, adv_out, small_sems.at[1]),
    ]
    for copy in last:
        copy.start()
    pltpu.make_async_copy(pred, pred, sem).wait()
    for copy in last:
        copy.wait()


def local(
    frames,
    owners,
    offsets,
    groups,
    latent,
    noise_blocks,
    rewards,
    embed_weight,
    norm_gain,
    mid_weight,
    head_weight,
):
    samples = frames.shape[0]
    slots, channels, width = latent.shape
    maxb = slots // samples
    peers = lax.axis_size("dp")
    mp = lax.axis_size("mp")
    features, hidden = mid_weight.shape
    pair_cap = (slots + peers - 1) // peers
    per_pair = (pair_cap + mp - 1) // mp
    total = peers * per_pair
    share = (slots + 2 * mp - 1) // (2 * mp)
    owner_rows = 3 * samples
    params = functools.partial(pltpu.CompilerParams, vmem_limit_bytes=48 * 1024 * 1024)
    step = next(n for n in (256, 128, hidden) if hidden % n == 0)

    combined, gram, send, block_x, block_n, picks, info = pl.pallas_call(
        functools.partial(start_kernel, maxb, per_pair, mp, step),
        in_specs=[HBM] * 11,
        out_specs=[VMEM] * 2 + [ANY] + [VMEM] * 4,
        out_shape=[
            jax.ShapeDtypeStruct((2 * channels, hidden), BF16),
            jax.ShapeDtypeStruct((3 * channels, channels), BF16),
            jax.ShapeDtypeStruct((peers, per_pair * channels + META, width), BF16),
            jax.ShapeDtypeStruct((share, channels, 2 * width), BF16),
            jax.ShapeDtypeStruct((share, channels, 2 * width), BF16),
            jax.ShapeDtypeStruct((2 * share, LANES), jnp.int32),
            jax.ShapeDtypeStruct((META, LANES), F32),
        ],
        scratch_shapes=[
            pltpu.SMEM((samples,), jnp.int32),
            pltpu.SMEM((slots,), jnp.int32),
            pltpu.SMEM((slots,), jnp.int32),
            pltpu.SMEM((samples,), jnp.int32),
            pltpu.SMEM((samples,), F32),
            pltpu.VMEM((channels, features), BF16),
            pltpu.VMEM((1, features), F32),
            pltpu.VMEM((features, hidden), BF16),
            pltpu.VMEM((peers, per_pair * channels + META, width), BF16),
            pltpu.SMEM((peers + 1,), jnp.int32),
            pltpu.SMEM((total + 1,), jnp.int32),
            pltpu.SMEM((total + 1,), jnp.int32),
            pltpu.SMEM((2 * share + 1,), jnp.int32),
            pltpu.SMEM((2 * share + 1,), jnp.int32),
            pltpu.SemaphoreType.DMA((5,)),
            pltpu.SemaphoreType.DMA((3,)),
            pltpu.SemaphoreType.DMA((hidden // step,)),
            pltpu.SemaphoreType.DMA((total,)),
            pltpu.SemaphoreType.DMA((2 * share,)),
            pltpu.SemaphoreType.DMA((2 * share,)),
            pltpu.SemaphoreType.DMA,
        ],
        compiler_params=params(),
        name="start",
    )(
        *map(
            in_hbm,
            (
                frames,
                owners,
                offsets,
                groups,
                rewards,
                latent,
                noise_blocks,
                embed_weight,
                norm_gain.reshape(1, features),
                mid_weight,
                head_weight.T,
            ),
        )
    )

    heads = [combined]
    near = mp
    while near > 1:
        near //= 2
        route = [(j, j ^ near) for j in range(mp)]
        more = []
        for head in heads:
            more.append(lax.ppermute(head, "mp", route))
        heads += more
    near = max(mp // 2, 1)
    recv = lax.all_to_all(send, "dp", split_axis=0, concat_axis=0, tiled=True)

    partial, halves, mt_near = pl.pallas_call(
        functools.partial(early_kernel, near, features),
        in_specs=[VMEM] * (2 + near),
        out_specs=[VMEM] * 3,
        out_shape=[
            jax.ShapeDtypeStruct((share, channels, 2 * width), F32),
            jax.ShapeDtypeStruct((share, 1, 2 * width), F32),
            jax.ShapeDtypeStruct((near * hidden, channels), BF16),
        ],
        compiler_params=params(),
        name="early",
    )(block_x, gram, *heads[:near])

    errs, mt_far = pl.pallas_call(
        functools.partial(errors_kernel, mp - near),
        in_specs=[VMEM] * (5 + mp - near),
        out_specs=[VMEM, VMEM],
        out_shape=[
            jax.ShapeDtypeStruct((1, LANES), F32),
            jax.ShapeDtypeStruct(((mp - near) * hidden, channels), BF16),
        ],
        compiler_params=params(),
        name="errors",
    )(picks, block_x, block_n, partial, halves, *heads[near:])

    tail = (peers + META - 1) // META * META + META
    payload = pl.pallas_call(
        functools.partial(owner_kernel, per_pair, near, mp, features),
        in_specs=[VMEM] * (5 + mp),
        out_specs=VMEM,
        out_shape=jax.ShapeDtypeStruct((total * channels + tail, width), BF16),
        scratch_shapes=[pltpu.SMEM((total + 1,), jnp.int32)],
        compiler_params=params(),
        name="owner",
    )(recv, errs, gram, mt_near, mt_far, *heads)

    gathered = lax.all_gather(payload, "mp", axis=0, tiled=False)

    return pl.pallas_call(
        functools.partial(place_kernel, per_pair, samples),
        in_specs=[VMEM] * 3,
        out_specs=[ANY] * 3,
        out_shape=[
            jax.ShapeDtypeStruct((owner_rows, channels, width), BF16),
            jax.ShapeDtypeStruct((samples,), F32),
            jax.ShapeDtypeStruct((samples,), F32),
        ],
        scratch_shapes=[
            pltpu.SMEM((samples,), F32),
            pltpu.SMEM((samples,), F32),
            pltpu.SemaphoreType.DMA((2,)),
            pltpu.SemaphoreType.DMA,
        ],
        compiler_params=params(),
        name="place",
    )(info, recv, gathered)


def solution(mesh):
    placed = (
        P("dp"),
        P("dp"),
        P("dp"),
        P("dp"),
        P("dp", None, None),
        P("dp", None, None),
        P("dp"),
        P(),
        P(),
        P(None, "mp"),
        P("mp", None),
    )
    mp = mesh.shape["mp"]
    near = mp
    while near > 1:
        near //= 2
    return jax.shard_map(
        local,
        mesh=mesh,
        in_specs=placed,
        out_specs=(P("dp", None, None), P("dp"), P("dp")),
        check_vma=False,
    )
```

```python
import functools

import jax
import jax.numpy as jnp
from jax import lax
from jax.experimental import pallas as pl
from jax.experimental.pallas import tpu as pltpu
from jax.sharding import PartitionSpec as P

GSIZE = 12
META = 8
LANES = 128
F32 = jnp.float32
BF16 = jnp.bfloat16
SMEM = pl.BlockSpec(memory_space=pltpu.SMEM)
VMEM = pl.BlockSpec(memory_space=pltpu.VMEM)
ANY = pl.BlockSpec(memory_space=pl.ANY)
HBM = pl.BlockSpec(memory_space=pltpu.HBM)


def in_hbm(value):
    return pltpu.with_memory_space_constraint(value, pltpu.HBM)


def split3(value):
    hi = value.astype(BF16)
    rest = value - hi.astype(F32)
    mid = rest.astype(BF16)
    lo = (rest - mid.astype(F32)).astype(BF16)
    return hi, mid, lo


def lane_row(scalars, count, dtype):
    lane = lax.broadcasted_iota(jnp.int32, (1, LANES), 1)
    row = jnp.zeros((1, LANES), dtype)
    for s in range(count):
        row = jnp.where(lane == s, scalars(s), row)
    return row


def live_count(frames, sample):
    return lax.shift_right_logical(frames[sample] - 1, 5) + 1


def rest_of(value, mp):
    return lax.bitwise_and(value, mp - 1) if mp & (mp - 1) == 0 else lax.rem(value, mp)


def part_of(value, mp):
    return lax.shift_right_logical(value, mp.bit_length() - 1) if mp & (mp - 1) == 0 else value // mp


def start_kernel(maxb, per_pair, peers, mp, step, *refs):
    (frames_h, owners_h, offsets_h, groups_h, rewards_h, latent, noise, embed_h, gain_h, weight, head_h) = refs[:11]
    (send, out, embed, block_x, block_n, picks, info) = refs[11:18]
    (frames, owners, offsets, groups, rewards, gain, held, blocks, meta, places, rows, source, chosen, slot_of) = refs[18:32]
    (small_sems, big_sems, weight_sems, row_sems, n_sems, meta_sem) = refs[32:]
    _, channels, width = latent.shape
    samples = frames.shape[0]
    share = block_x.shape[0] * 2
    total = peers * per_pair
    small = [
        pltpu.make_async_copy(a, b, small_sems.at[n])
        for n, (a, b) in enumerate(
            [
                (frames_h, frames),
                (owners_h, owners),
                (offsets_h, offsets),
                (groups_h, groups),
                (rewards_h, rewards),
            ]
        )
    ]
    big = [
        pltpu.make_async_copy(embed_h, embed, big_sems.at[0]),
        pltpu.make_async_copy(gain_h, gain, big_sems.at[1]),
        pltpu.make_async_copy(latent, blocks, big_sems.at[2]),
        pltpu.make_async_copy(head_h, out.at[pl.ds(channels, channels)], big_sems.at[3]),
    ]
    parts = [
        pltpu.make_async_copy(weight.at[pl.ds(n, step)], held.at[pl.ds(n, step)], weight_sems.at[n // step])
        for n in range(0, weight.shape[0], step)
    ]
    for copy in small + big[:3] + parts + big[3:]:
        copy.start()

    me = lax.axis_index("mp")
    shift = rest_of(me + mp - rest_of(lax.axis_index("dp"), mp), mp)
    for o in range(peers + 1):
        places[o] = 0
    for n in range(total + 1):
        rows[n] = 0
        source[n] = 0
    for j in range(share + 1):
        chosen[j] = 0
        slot_of[j] = 0
    for copy in small + big[:3]:
        copy.wait()
    seen = jnp.int32(0)
    count = jnp.int32(0)
    for s in range(samples):
        live_here = live_count(frames, s)
        for k in range(maxb):
            i = s * maxb + k
            live = k < live_here
            o = jnp.where(live, owners[i], peers)
            place = places[o]
            places[o] = place + 1
            q = part_of(place, mp)
            goes = live & (rest_of(place, mp) == shift) & (q < per_pair)
            n = jnp.where(goes, o * per_pair + q, total)
            rows[n] = offsets[i] + 1
            source[n] = i
            chosen[count] = s
            slot_of[count] = i
            mine = live & (rest_of(seen, mp) == me)
            seen = seen + live.astype(jnp.int32)
            count = count + mine.astype(jnp.int32)

    copies = [
        pltpu.make_async_copy(
            blocks.at[source[o * per_pair + q]],
            send.at[o, pl.ds(q * channels, channels)],
            row_sems.at[o * per_pair + q],
        )
        for o in range(peers)
        for q in range(per_pair)
    ]
    for j in range(share):
        copies.append(
            pltpu.make_async_copy(
                noise.at[slot_of[j]], block_n.at[j // 2, :, pl.ds(j % 2 * width, width)], n_sems.at[j]
            )
        )
    for copy in copies:
        copy.start()
    for j in range(share):
        block_x[j // 2, :, j % 2 * width : (j % 2 + 1) * width] = blocks[slot_of[j]]

    sub = lax.broadcasted_iota(jnp.int32, picks.shape, 0)
    found = jnp.full(picks.shape, -1, jnp.int32)
    for j in range(share):
        found = jnp.where((sub == j) & (j < count), chosen[j], found)
    picks[...] = found

    reward = lane_row(lambda s: rewards[s], samples, F32)
    group = lane_row(lambda s: groups[s].astype(F32), samples, F32)
    counts = lane_row(lambda s: live_count(frames, s).astype(F32), samples, F32)
    hi, mid, lo = split3(reward)
    sub = lax.broadcasted_iota(jnp.int32, (META, LANES), 0)
    info[...] = jnp.where(sub == 0, reward, jnp.where(sub == 1, group, counts))
    shared = jnp.where(sub == 1, hi.astype(F32), 0.0)
    shared = jnp.where(sub == 2, mid.astype(F32), shared)
    shared = jnp.where(sub == 3, lo.astype(F32), shared)
    shared = jnp.where(sub == 4, group, shared)
    for o in range(peers):
        first = lane_row(lambda q: rows[o * per_pair + q].astype(F32), per_pair, F32)
        meta[o] = jnp.where(sub == 0, first, shared).astype(BF16)
    copies.append(pltpu.make_async_copy(meta, send.at[:, pl.ds(per_pair * channels, META)], meta_sem))
    copies[-1].start()

    scaled = embed[...].astype(F32) * gain[...]
    hi = scaled.astype(BF16)
    lo = (scaled - hi.astype(F32)).astype(BF16)
    both = jnp.concatenate([hi, lo], axis=0)
    total_m = None
    for n, copy in enumerate(parts):
        copy.wait()
        part = slice(n * step, (n + 1) * step)
        m = jnp.dot(both[:, part], held[part, :], preferred_element_type=F32)
        total_m = m if total_m is None else total_m + m
    out[:channels, :] = (total_m[:channels] + total_m[channels:]).astype(BF16)
    for copy in big[3:] + copies:
        copy.wait()


def norm_factors(xs, gram, features):
    channels, width = xs[0].shape
    x = jnp.concatenate(xs, axis=1)
    g = jnp.dot(gram, x, preferred_element_type=F32)
    gx = g[:channels] + g[channels : 2 * channels] + g[2 * channels :]
    mean_sq = jnp.sum(gx * x.astype(F32), axis=0, keepdims=True) * (1.0 / features)
    half = 0.5 * lax.rsqrt(jnp.maximum(mean_sq, 0.0) + 0.25)
    return [half[:, p * width : (p + 1) * width] for p in range(len(xs))]


def velocities(xs, halves, parts, totals):
    totals = list(totals)
    waiting = []

    def finish():
        p, head, act = waiting.pop()
        part = jnp.dot(head, act, preferred_element_type=F32)
        totals[p] = part if totals[p] is None else totals[p] + part

    for p, x in enumerate(xs):
        for mt, both, row in parts:
            channels, hidden = both.shape[0] // 2, both.shape[1]
            mid = jnp.dot(mt[row : row + hidden, :], x, preferred_element_type=F32)
            if waiting:
                finish()
            v = mid * halves[p]
            waiting.append((p, both[channels:, :], (v + v * jnp.tanh(v)).astype(BF16)))
    finish()
    return totals


def turn(mt, heads):
    channels, hidden = heads[0].shape[0] // 2, heads[0].shape[1]
    for m, head in enumerate(heads):
        mt[m * hidden : (m + 1) * hidden, :] = head[:channels, :].T


def shards_of(mt, heads):
    hidden = heads[0].shape[1]
    return [(mt, head, m * hidden) for m, head in enumerate(heads)]


def early_kernel(near, features, block_x, embed, *refs):
    heads, (partial, halves, mt, gram) = refs[:near], refs[near:]
    e = embed[...]
    hi, mid, lo = split3(lax.dot_general(e, e, (((1,), (1,)), ((), ())), preferred_element_type=F32))
    gram[...] = jnp.concatenate([hi, mid, lo], axis=0)
    turn(mt, heads)
    xs = [block_x[p] for p in range(block_x.shape[0])]
    half = norm_factors(xs, gram[...], features)
    for p, total in enumerate(velocities(xs, half, shards_of(mt, heads), [None] * len(xs))):
        halves[p] = half[p]
        partial[p] = total


def errors_kernel(far, picks, block_x, block_n, partial, halves, *refs):
    heads, (errs, mt) = refs[:far], refs[far:]
    pairs, _, double = block_x.shape
    width = double // 2
    turn(mt, heads)
    xs = [block_x[p] for p in range(pairs)]
    half = [halves[p] for p in range(pairs)]
    totals = velocities(xs, half, shards_of(mt, heads), [partial[p] for p in range(pairs)])
    sub = lax.broadcasted_iota(jnp.int32, picks.shape, 0)
    lane = lax.broadcasted_iota(jnp.int32, picks.shape, 1)
    sums = jnp.zeros(picks.shape, F32)
    for p, v in enumerate(totals):
        e = block_n[p].astype(F32) + v
        line = jnp.sum(e * e, axis=0, keepdims=True)
        sums = jnp.where(sub == 2 * p, line[:, :width], sums)
        sums = jnp.where(sub == 2 * p + 1, line[:, width:], sums)
    each = jnp.sum(sums, axis=1, keepdims=True)
    errs[...] = jnp.sum(jnp.where(lane == picks[...], each, 0.0), axis=0, keepdims=True)


def owner_kernel(per_pair, near, shards, features, recv, errs, gram, mt_near, mt_far, *refs):
    heads, (out, order) = refs[:shards], refs[shards:]
    peers = recv.shape[0]
    channels = heads[0].shape[0] // 2
    total = peers * per_pair
    base = total * channels
    first = recv[:, per_pair * channels, :].astype(F32)
    out[base : base + peers, :] = first.astype(BF16)
    hi, mid, lo = split3(errs[...])
    sub = lax.broadcasted_iota(jnp.int32, (META, LANES), 0)
    meta = jnp.where(sub == 0, hi.astype(F32), 0.0)
    meta = jnp.where(sub == 1, mid.astype(F32), meta)
    meta = jnp.where(sub == 2, lo.astype(F32), meta)
    out[out.shape[0] - META :, :] = meta.astype(BF16)
    lane = lax.broadcasted_iota(jnp.int32, (peers, LANES), 1)
    number = lax.broadcasted_iota(jnp.int32, (peers, LANES), 0) * per_pair + lane
    count = jnp.int32(0)
    for low in range(0, total, 16):
        inside = (lane < per_pair) & (number >= low) & (number < low + 16) & (first > 0)
        bits = jnp.where(inside, lax.shift_left(1, jnp.clip(number - low, 0, 15)).astype(F32), 0.0)
        mask = jnp.sum(bits).astype(jnp.int32)
        for n in range(low, min(low + 16, total)):
            order[count] = n
            count = count + lax.bitwise_and(lax.shift_right_logical(mask, n - low), 1)
    parts = shards_of(mt_near, heads[:near]) + shards_of(mt_far, heads[near:])

    def block_of(n):
        if per_pair == 1:
            return recv[n, :channels, :]
        return recv[n // per_pair, pl.ds(pl.multiple_of((n % per_pair) * channels, channels), channels), :]

    def run(begin, pairs):
        slots = [order[jnp.minimum(begin + j, count - 1)] for j in range(2 * pairs)]
        xs = [
            jnp.concatenate([block_of(slots[2 * p]), block_of(slots[2 * p + 1])], axis=1)
            for p in range(pairs)
        ]
        half = norm_factors(xs, gram[...], features)
        for p, v in enumerate(velocities(xs, half, parts, [None] * pairs)):
            v = v.astype(BF16)
            width = v.shape[1] // 2
            for j in range(2):
                at = pl.multiple_of(slots[2 * p + j] * channels, channels)
                out[pl.ds(at, channels), :] = v[:, j * width : (j + 1) * width]

    def quad(n, carry):
        left = (jnp.clip(count - 8 * n, 0, 8) + 1) // 2
        for pairs in range(1, 5):

            @pl.when(left == pairs)
            def _():
                run(8 * n, pairs)

        return carry

    if total <= 8:
        quad(0, 0)
    else:
        lax.fori_loop(0, (total + 7) // 8, quad, 0)


def place_kernel(per_pair, samples, info, recv, gathered, pred, log_out, adv_out, log_prob, advantage, small_sems, sem):
    shards = gathered.shape[0]
    rows_here, channels, width = pred.shape
    peers = recv.shape[0]
    total = peers * per_pair
    base = total * channels
    bits = rows_here.bit_length()
    pack = 24 // bits
    lane8 = lax.broadcasted_iota(jnp.int32, (peers, LANES), 1)
    number = lax.broadcasted_iota(jnp.int32, (peers, LANES), 0) * per_pair + lane8
    scale = lax.shift_left(1, bits * lax.rem(number, pack)).astype(F32)
    for m in range(shards):
        first = gathered[m, base : base + peers, :].astype(F32)
        for low in range(0, total, pack):
            inside = (lane8 < per_pair) & (number >= low) & (number < low + pack)
            code = jnp.sum(jnp.where(inside, first * scale, 0.0)).astype(jnp.int32)
            for n in range(low, min(low + pack, total)):
                row = lax.bitwise_and(lax.shift_right_logical(code, bits * (n - low)), 2**bits - 1)

                @pl.when(row > 0)
                def _():
                    pltpu.make_async_copy(
                        gathered.at[m, pl.ds(n * channels, channels)], pred.at[row - 1], sem
                    ).start()

    lane = lax.broadcasted_iota(jnp.int32, (1, LANES), 1)
    sums = jnp.zeros((1, LANES), F32)
    for m in range(shards):
        part = gathered[m, gathered.shape[1] - META :, :].astype(F32)
        sums = sums + (part[0:1] + part[1:2] + part[2:3])
    reward, own_group, counts = info[0:1, :], info[1:2, :], info[2:3, :]
    size = jnp.where(lane < samples, counts * float(channels * width), 1.0)
    logs = -0.5 * sums / size

    meta = recv[:, pl.ds(per_pair * channels, META), :].astype(F32)
    every = meta[:, 1, :] + meta[:, 2, :] + meta[:, 3, :]
    group = jnp.where(lax.broadcasted_iota(jnp.int32, every.shape, 1) < samples, meta[:, 4, :], -1.0)
    mean = jnp.zeros((1, LANES), F32)
    meansq = jnp.zeros((1, LANES), F32)
    for s in range(samples):
        mine = jnp.sum(jnp.where(lane == s, own_group, 0.0), axis=1, keepdims=True)
        chosen = group == mine
        one = jnp.sum(jnp.sum(jnp.where(chosen, every, 0.0), axis=0, keepdims=True), axis=1, keepdims=True)
        two = jnp.sum(jnp.sum(jnp.where(chosen, every * every, 0.0), axis=0, keepdims=True), axis=1, keepdims=True)
        mean = jnp.where(lane == s, one / GSIZE, mean)
        meansq = jnp.where(lane == s, two / GSIZE, meansq)
    scores = (reward - mean) / jnp.sqrt(meansq - mean * mean + 0.25)
    for s in range(samples):
        advantage[s] = jnp.sum(jnp.where(lane == s, scores, 0.0))
        log_prob[s] = jnp.sum(jnp.where(lane == s, logs, 0.0))
    last = [
        pltpu.make_async_copy(log_prob, log_out, small_sems.at[0]),
        pltpu.make_async_copy(advantage, adv_out, small_sems.at[1]),
    ]
    for copy in last:
        copy.start()
    pltpu.make_async_copy(pred, pred, sem).wait()
    for copy in last:
        copy.wait()


def local(
    frames,
    owners,
    offsets,
    groups,
    latent,
    noise_blocks,
    rewards,
    embed_weight,
    norm_gain,
    mid_weight,
    head_weight,
):
    samples = frames.shape[0]
    slots, channels, width = latent.shape
    maxb = slots // samples
    peers = lax.axis_size("dp")
    mp = lax.axis_size("mp")
    features, hidden = mid_weight.shape
    pair_cap = (slots + peers - 1) // peers
    per_pair = (pair_cap + mp - 1) // mp
    total = peers * per_pair
    share = (slots + 2 * mp - 1) // (2 * mp)
    owner_rows = 3 * samples
    params = functools.partial(pltpu.CompilerParams, vmem_limit_bytes=48 * 1024 * 1024)
    step = next(features // n for n in (3, 2, 1) if features % (128 * n) == 0 or n == 1)

    send, combined, embed, block_x, block_n, picks, info = pl.pallas_call(
        functools.partial(start_kernel, maxb, per_pair, peers, mp, step),
        in_specs=[HBM] * 11,
        out_specs=[ANY] + [VMEM] * 6,
        out_shape=[
            jax.ShapeDtypeStruct((peers, per_pair * channels + META, width), BF16),
            jax.ShapeDtypeStruct((2 * channels, hidden), BF16),
            jax.ShapeDtypeStruct((channels, features), BF16),
            jax.ShapeDtypeStruct((share, channels, 2 * width), BF16),
            jax.ShapeDtypeStruct((share, channels, 2 * width), BF16),
            jax.ShapeDtypeStruct((2 * share, LANES), jnp.int32),
            jax.ShapeDtypeStruct((META, LANES), F32),
        ],
        scratch_shapes=[
            pltpu.SMEM((samples,), jnp.int32),
            pltpu.SMEM((slots,), jnp.int32),
            pltpu.SMEM((slots,), jnp.int32),
            pltpu.SMEM((samples,), jnp.int32),
            pltpu.SMEM((samples,), F32),
            pltpu.VMEM((1, features), F32),
            pltpu.VMEM((features, hidden), BF16),
            pltpu.VMEM((slots, channels, width), BF16),
            pltpu.VMEM((peers, META, width), BF16),
            pltpu.SMEM((peers + 1,), jnp.int32),
            pltpu.SMEM((total + 1,), jnp.int32),
            pltpu.SMEM((total + 1,), jnp.int32),
            pltpu.SMEM((2 * share + 1,), jnp.int32),
            pltpu.SMEM((2 * share + 1,), jnp.int32),
            pltpu.SemaphoreType.DMA((5,)),
            pltpu.SemaphoreType.DMA((4,)),
            pltpu.SemaphoreType.DMA((features // step,)),
            pltpu.SemaphoreType.DMA((total,)),
            pltpu.SemaphoreType.DMA((2 * share,)),
            pltpu.SemaphoreType.DMA,
        ],
        compiler_params=params(),
        name="start",
    )(
        *map(
            in_hbm,
            (
                frames,
                owners,
                offsets,
                groups,
                rewards,
                latent,
                noise_blocks,
                embed_weight,
                norm_gain.reshape(1, features),
                mid_weight,
                head_weight.T,
            ),
        )
    )

    def swapped(value, axis, count, bit):
        return lax.ppermute(value, axis, [(j, j ^ bit) for j in range(count)])

    recv = lax.all_to_all(send, "dp", split_axis=0, concat_axis=0, tiled=True)
    heads = [combined, swapped(combined, "mp", mp, mp // 2)]
    for n in range(1, mp // 2):
        heads += [swapped(head, "mp", mp, n) for head in heads[:2]]
    near = 2

    partial, halves, mt_near, gram = pl.pallas_call(
        functools.partial(early_kernel, near, features),
        in_specs=[VMEM] * (2 + near),
        out_specs=[VMEM] * 4,
        out_shape=[
            jax.ShapeDtypeStruct((share, channels, 2 * width), F32),
            jax.ShapeDtypeStruct((share, 1, 2 * width), F32),
            jax.ShapeDtypeStruct((near * hidden, channels), BF16),
            jax.ShapeDtypeStruct((3 * channels, channels), BF16),
        ],
        compiler_params=params(),
        name="early",
    )(block_x, embed, *heads[:near])

    errs, mt_far = pl.pallas_call(
        functools.partial(errors_kernel, mp - near),
        in_specs=[VMEM] * (5 + mp - near),
        out_specs=[VMEM, VMEM],
        out_shape=[
            jax.ShapeDtypeStruct((1, LANES), F32),
            jax.ShapeDtypeStruct(((mp - near) * hidden, channels), BF16),
        ],
        compiler_params=params(),
        name="errors",
    )(picks, block_x, block_n, partial, halves, *heads[near:])

    tail = (peers + META - 1) // META * META + META
    payload = pl.pallas_call(
        functools.partial(owner_kernel, per_pair, near, mp, features),
        in_specs=[VMEM] * (5 + mp),
        out_specs=VMEM,
        out_shape=jax.ShapeDtypeStruct((total * channels + tail, width), BF16),
        scratch_shapes=[pltpu.SMEM((total + 1,), jnp.int32)],
        compiler_params=params(),
        name="owner",
    )(recv, errs, gram, mt_near, mt_far, *heads)

    gathered = lax.all_gather(payload, "mp", axis=0, tiled=False)

    return pl.pallas_call(
        functools.partial(place_kernel, per_pair, samples),
        in_specs=[VMEM] * 3,
        out_specs=[ANY] * 3,
        out_shape=[
            jax.ShapeDtypeStruct((owner_rows, channels, width), BF16),
            jax.ShapeDtypeStruct((samples,), F32),
            jax.ShapeDtypeStruct((samples,), F32),
        ],
        scratch_shapes=[
            pltpu.SMEM((samples,), F32),
            pltpu.SMEM((samples,), F32),
            pltpu.SemaphoreType.DMA((2,)),
            pltpu.SemaphoreType.DMA,
        ],
        compiler_params=params(),
        name="place",
    )(info, recv, gathered)


def solution(mesh):
    placed = (
        P("dp"),
        P("dp"),
        P("dp"),
        P("dp"),
        P("dp", None, None),
        P("dp", None, None),
        P("dp"),
        P(),
        P(),
        P(None, "mp"),
        P("mp", None),
    )
    return jax.shard_map(
        local,
        mesh=mesh,
        in_specs=placed,
        out_specs=(P("dp", None, None), P("dp"), P("dp")),
        check_vma=False,
    )
```

```python
import functools

import jax
import jax.numpy as jnp
from jax import lax
from jax.experimental import pallas as pl
from jax.experimental.pallas import tpu as pltpu
from jax.sharding import PartitionSpec as P

GSIZE = 12
META = 8
LANES = 128
F32 = jnp.float32
BF16 = jnp.bfloat16
SMEM = pl.BlockSpec(memory_space=pltpu.SMEM)
VMEM = pl.BlockSpec(memory_space=pltpu.VMEM)
ANY = pl.BlockSpec(memory_space=pl.ANY)
HBM = pl.BlockSpec(memory_space=pltpu.HBM)


def in_hbm(value):
    return pltpu.with_memory_space_constraint(value, pltpu.HBM)


def split3(value):
    hi = value.astype(BF16)
    rest = value - hi.astype(F32)
    mid = rest.astype(BF16)
    lo = (rest - mid.astype(F32)).astype(BF16)
    return hi, mid, lo


def lane_row(scalars, count, dtype):
    lane = lax.broadcasted_iota(jnp.int32, (1, LANES), 1)
    row = jnp.zeros((1, LANES), dtype)
    for s in range(count):
        row = jnp.where(lane == s, scalars(s), row)
    return row


def live_count(frames, sample):
    return lax.shift_right_logical(frames[sample] - 1, 5) + 1


def rest_of(value, mp):
    return lax.bitwise_and(value, mp - 1) if mp & (mp - 1) == 0 else lax.rem(value, mp)


def part_of(value, mp):
    return lax.shift_right_logical(value, mp.bit_length() - 1) if mp & (mp - 1) == 0 else value // mp


def start_kernel(maxb, per_pair, peers, mp, step, *refs):
    (frames_h, owners_h, offsets_h, groups_h, rewards_h, latent, noise, embed_h, gain_h, weight, head_h) = refs[:11]
    (send, out, embed, block_x, block_n, picks, info) = refs[11:18]
    (frames, owners, offsets, groups, rewards, gain, held, blocks, meta, places, rows, source, chosen, slot_of) = refs[18:32]
    (small_sems, big_sems, weight_sems, row_sems, n_sems, meta_sem) = refs[32:]
    _, channels, width = latent.shape
    samples = frames.shape[0]
    share = block_x.shape[0] * 2
    total = peers * per_pair
    small = [
        pltpu.make_async_copy(a, b, small_sems.at[n])
        for n, (a, b) in enumerate(
            [
                (frames_h, frames),
                (owners_h, owners),
                (offsets_h, offsets),
                (groups_h, groups),
                (rewards_h, rewards),
            ]
        )
    ]
    big = [
        pltpu.make_async_copy(embed_h, embed, big_sems.at[0]),
        pltpu.make_async_copy(gain_h, gain, big_sems.at[1]),
        pltpu.make_async_copy(latent, blocks, big_sems.at[2]),
        pltpu.make_async_copy(head_h, out.at[pl.ds(channels, channels)], big_sems.at[3]),
    ]
    parts = [
        pltpu.make_async_copy(weight.at[pl.ds(n, step)], held.at[pl.ds(n, step)], weight_sems.at[n // step])
        for n in range(0, weight.shape[0], step)
    ]
    for copy in small + big[:3] + parts + big[3:]:
        copy.start()

    me = lax.axis_index("mp")
    shift = rest_of(me + mp - rest_of(lax.axis_index("dp"), mp), mp)
    for o in range(peers + 1):
        places[o] = 0
    for n in range(total + 1):
        rows[n] = 0
        source[n] = 0
    for j in range(share + 1):
        chosen[j] = 0
        slot_of[j] = 0
    for copy in small + big[:3]:
        copy.wait()
    seen = jnp.int32(0)
    count = jnp.int32(0)
    for s in range(samples):
        live_here = live_count(frames, s)
        for k in range(maxb):
            i = s * maxb + k
            live = k < live_here
            o = jnp.where(live, owners[i], peers)
            place = places[o]
            places[o] = place + 1
            q = part_of(place, mp)
            goes = live & (rest_of(place, mp) == shift) & (q < per_pair)
            n = jnp.where(goes, o * per_pair + q, total)
            rows[n] = offsets[i] + 1
            source[n] = i
            chosen[count] = s
            slot_of[count] = i
            mine = live & (rest_of(seen, mp) == me)
            seen = seen + live.astype(jnp.int32)
            count = count + mine.astype(jnp.int32)

    copies = [
        pltpu.make_async_copy(
            blocks.at[source[o * per_pair + q]],
            send.at[o, pl.ds(q * channels, channels)],
            row_sems.at[o * per_pair + q],
        )
        for o in range(peers)
        for q in range(per_pair)
    ]
    for j in range(share):
        copies.append(
            pltpu.make_async_copy(
                noise.at[slot_of[j]], block_n.at[j // 2, :, pl.ds(j % 2 * width, width)], n_sems.at[j]
            )
        )
    for copy in copies:
        copy.start()
    for j in range(share):
        block_x[j // 2, :, j % 2 * width : (j % 2 + 1) * width] = blocks[slot_of[j]]

    sub = lax.broadcasted_iota(jnp.int32, picks.shape, 0)
    found = jnp.full(picks.shape, -1, jnp.int32)
    for j in range(share):
        found = jnp.where((sub == j) & (j < count), chosen[j], found)
    picks[...] = found

    reward = lane_row(lambda s: rewards[s], samples, F32)
    group = lane_row(lambda s: groups[s].astype(F32), samples, F32)
    counts = lane_row(lambda s: live_count(frames, s).astype(F32), samples, F32)
    hi, mid, lo = split3(reward)
    sub = lax.broadcasted_iota(jnp.int32, (META, LANES), 0)
    info[...] = jnp.where(sub == 0, reward, jnp.where(sub == 1, group, counts))
    shared = jnp.where(sub == 1, hi.astype(F32), 0.0)
    shared = jnp.where(sub == 2, mid.astype(F32), shared)
    shared = jnp.where(sub == 3, lo.astype(F32), shared)
    shared = jnp.where(sub == 4, group, shared)
    for o in range(peers):
        first = lane_row(lambda q: rows[o * per_pair + q].astype(F32), per_pair, F32)
        meta[o] = jnp.where(sub == 0, first, shared).astype(BF16)
    copies.append(pltpu.make_async_copy(meta, send.at[:, pl.ds(per_pair * channels, META)], meta_sem))
    copies[-1].start()

    scaled = embed[...].astype(F32) * gain[...]
    hi = scaled.astype(BF16)
    lo = (scaled - hi.astype(F32)).astype(BF16)
    both = jnp.concatenate([hi, lo], axis=0)
    total_m = None
    for n, copy in enumerate(parts):
        copy.wait()
        part = slice(n * step, (n + 1) * step)
        m = jnp.dot(both[:, part], held[part, :], preferred_element_type=F32)
        total_m = m if total_m is None else total_m + m
    out[:channels, :] = (total_m[:channels] + total_m[channels:]).astype(BF16)
    for copy in big[3:] + copies:
        copy.wait()


def norm_factors(xs, gram, features):
    channels, width = xs[0].shape
    x = jnp.concatenate(xs, axis=1)
    g = jnp.dot(gram, x, preferred_element_type=F32)
    gx = g[:channels] + g[channels : 2 * channels] + g[2 * channels :]
    mean_sq = jnp.sum(gx * x.astype(F32), axis=0, keepdims=True) * (1.0 / features)
    half = 0.5 * lax.rsqrt(jnp.maximum(mean_sq, 0.0) + 0.25)
    return [half[:, p * width : (p + 1) * width] for p in range(len(xs))]


def velocities(xs, halves, parts, totals):
    totals = list(totals)
    waiting = []

    def finish():
        p, head, act = waiting.pop()
        part = jnp.dot(head, act, preferred_element_type=F32)
        totals[p] = part if totals[p] is None else totals[p] + part

    for p, x in enumerate(xs):
        exact = x.astype(F32) * halves[p]
        hi = exact.astype(BF16)
        lo = (exact - hi.astype(F32)).astype(BF16)
        x = jnp.concatenate([hi, lo], axis=0)
        for mt, both, row in parts:
            channels, hidden = both.shape[0] // 2, both.shape[1]
            v = jnp.dot(mt[row : row + hidden, :], x, preferred_element_type=F32)
            if waiting:
                finish()
            waiting.append((p, both[channels:, :], (v + v * jnp.tanh(v)).astype(BF16)))
    finish()
    return totals


def turn(mt, heads):
    channels, hidden = heads[0].shape[0] // 2, heads[0].shape[1]
    for m, head in enumerate(heads):
        mt[m * hidden : (m + 1) * hidden, :] = jnp.concatenate([head[:channels, :]] * 2, axis=0).T


def shards_of(mt, heads):
    hidden = heads[0].shape[1]
    return [(mt, head, m * hidden) for m, head in enumerate(heads)]


def early_kernel(near, features, block_x, embed, *refs):
    heads, (partial, halves, mt, gram) = refs[:near], refs[near:]
    e = embed[...]
    hi, mid, lo = split3(lax.dot_general(e, e, (((1,), (1,)), ((), ())), preferred_element_type=F32))
    gram[...] = jnp.concatenate([hi, mid, lo], axis=0)
    turn(mt, heads)
    xs = [block_x[p] for p in range(block_x.shape[0])]
    half = norm_factors(xs, gram[...], features)
    for p, total in enumerate(velocities(xs, half, shards_of(mt, heads), [None] * len(xs))):
        halves[p] = half[p]
        partial[p] = total


def errors_kernel(far, picks, block_x, block_n, partial, halves, *refs):
    heads, (errs, mt) = refs[:far], refs[far:]
    pairs, _, double = block_x.shape
    width = double // 2
    turn(mt, heads)
    xs = [block_x[p] for p in range(pairs)]
    half = [halves[p] for p in range(pairs)]
    totals = velocities(xs, half, shards_of(mt, heads), [partial[p] for p in range(pairs)])
    sub = lax.broadcasted_iota(jnp.int32, picks.shape, 0)
    lane = lax.broadcasted_iota(jnp.int32, picks.shape, 1)
    sums = jnp.zeros(picks.shape, F32)
    for p, v in enumerate(totals):
        e = block_n[p].astype(F32) + v
        line = jnp.sum(e * e, axis=0, keepdims=True)
        sums = jnp.where(sub == 2 * p, line[:, :width], sums)
        sums = jnp.where(sub == 2 * p + 1, line[:, width:], sums)
    each = jnp.sum(sums, axis=1, keepdims=True)
    errs[...] = jnp.sum(jnp.where(lane == picks[...], each, 0.0), axis=0, keepdims=True)


def owner_kernel(per_pair, near, shards, features, recv, errs, gram, mt_near, mt_far, *refs):
    heads, (out, order) = refs[:shards], refs[shards:]
    peers = recv.shape[0]
    channels = heads[0].shape[0] // 2
    total = peers * per_pair
    base = total * channels
    first = recv[:, per_pair * channels, :].astype(F32)
    out[base : base + peers, :] = first.astype(BF16)
    hi, mid, lo = split3(errs[...])
    sub = lax.broadcasted_iota(jnp.int32, (META, LANES), 0)
    meta = jnp.where(sub == 0, hi.astype(F32), 0.0)
    meta = jnp.where(sub == 1, mid.astype(F32), meta)
    meta = jnp.where(sub == 2, lo.astype(F32), meta)
    out[out.shape[0] - META :, :] = meta.astype(BF16)
    lane = lax.broadcasted_iota(jnp.int32, (peers, LANES), 1)
    number = lax.broadcasted_iota(jnp.int32, (peers, LANES), 0) * per_pair + lane
    count = jnp.int32(0)
    for low in range(0, total, 16):
        inside = (lane < per_pair) & (number >= low) & (number < low + 16) & (first > 0)
        bits = jnp.where(inside, lax.shift_left(1, jnp.clip(number - low, 0, 15)).astype(F32), 0.0)
        mask = jnp.sum(bits).astype(jnp.int32)
        for n in range(low, min(low + 16, total)):
            order[count] = n
            count = count + lax.bitwise_and(lax.shift_right_logical(mask, n - low), 1)
    parts = shards_of(mt_near, heads[:near]) + shards_of(mt_far, heads[near:])

    def block_of(n):
        if per_pair == 1:
            return recv[n, :channels, :]
        return recv[n // per_pair, pl.ds(pl.multiple_of((n % per_pair) * channels, channels), channels), :]

    def run(begin, pairs):
        slots = [order[jnp.minimum(begin + j, count - 1)] for j in range(2 * pairs)]
        xs = [
            jnp.concatenate([block_of(slots[2 * p]), block_of(slots[2 * p + 1])], axis=1)
            for p in range(pairs)
        ]
        half = norm_factors(xs, gram[...], features)
        for p, v in enumerate(velocities(xs, half, parts, [None] * pairs)):
            v = v.astype(BF16)
            width = v.shape[1] // 2
            for j in range(2):
                at = pl.multiple_of(slots[2 * p + j] * channels, channels)
                out[pl.ds(at, channels), :] = v[:, j * width : (j + 1) * width]

    def quad(n, carry):
        left = (jnp.clip(count - 8 * n, 0, 8) + 1) // 2
        for pairs in range(1, 5):

            @pl.when(left == pairs)
            def _():
                run(8 * n, pairs)

        return carry

    if total <= 8:
        quad(0, 0)
    else:
        lax.fori_loop(0, (total + 7) // 8, quad, 0)


def place_kernel(per_pair, samples, info, recv, gathered, pred, log_out, adv_out, log_prob, advantage, small_sems, sem):
    shards = gathered.shape[0]
    rows_here, channels, width = pred.shape
    peers = recv.shape[0]
    total = peers * per_pair
    base = total * channels
    bits = rows_here.bit_length()
    pack = 24 // bits
    lane8 = lax.broadcasted_iota(jnp.int32, (peers, LANES), 1)
    number = lax.broadcasted_iota(jnp.int32, (peers, LANES), 0) * per_pair + lane8
    scale = lax.shift_left(1, bits * lax.rem(number, pack)).astype(F32)
    for m in range(shards):
        first = gathered[m, base : base + peers, :].astype(F32)
        for low in range(0, total, pack):
            inside = (lane8 < per_pair) & (number >= low) & (number < low + pack)
            code = jnp.sum(jnp.where(inside, first * scale, 0.0)).astype(jnp.int32)
            for n in range(low, min(low + pack, total)):
                row = lax.bitwise_and(lax.shift_right_logical(code, bits * (n - low)), 2**bits - 1)

                @pl.when(row > 0)
                def _():
                    pltpu.make_async_copy(
                        gathered.at[m, pl.ds(n * channels, channels)], pred.at[row - 1], sem
                    ).start()

    lane = lax.broadcasted_iota(jnp.int32, (1, LANES), 1)
    sums = jnp.zeros((1, LANES), F32)
    for m in range(shards):
        part = gathered[m, gathered.shape[1] - META :, :].astype(F32)
        sums = sums + (part[0:1] + part[1:2] + part[2:3])
    reward, own_group, counts = info[0:1, :], info[1:2, :], info[2:3, :]
    size = jnp.where(lane < samples, counts * float(channels * width), 1.0)
    logs = -0.5 * sums / size

    meta = recv[:, pl.ds(per_pair * channels, META), :].astype(F32)
    every = meta[:, 1, :] + meta[:, 2, :] + meta[:, 3, :]
    group = jnp.where(lax.broadcasted_iota(jnp.int32, every.shape, 1) < samples, meta[:, 4, :], -1.0)
    mean = jnp.zeros((1, LANES), F32)
    meansq = jnp.zeros((1, LANES), F32)
    for s in range(samples):
        mine = jnp.sum(jnp.where(lane == s, own_group, 0.0), axis=1, keepdims=True)
        chosen = group == mine
        one = jnp.sum(jnp.sum(jnp.where(chosen, every, 0.0), axis=0, keepdims=True), axis=1, keepdims=True)
        two = jnp.sum(jnp.sum(jnp.where(chosen, every * every, 0.0), axis=0, keepdims=True), axis=1, keepdims=True)
        mean = jnp.where(lane == s, one / GSIZE, mean)
        meansq = jnp.where(lane == s, two / GSIZE, meansq)
    scores = (reward - mean) / jnp.sqrt(meansq - mean * mean + 0.25)
    for s in range(samples):
        advantage[s] = jnp.sum(jnp.where(lane == s, scores, 0.0))
        log_prob[s] = jnp.sum(jnp.where(lane == s, logs, 0.0))
    last = [
        pltpu.make_async_copy(log_prob, log_out, small_sems.at[0]),
        pltpu.make_async_copy(advantage, adv_out, small_sems.at[1]),
    ]
    for copy in last:
        copy.start()
    pltpu.make_async_copy(pred, pred, sem).wait()
    for copy in last:
        copy.wait()


def local(
    frames,
    owners,
    offsets,
    groups,
    latent,
    noise_blocks,
    rewards,
    embed_weight,
    norm_gain,
    mid_weight,
    head_weight,
):
    samples = frames.shape[0]
    slots, channels, width = latent.shape
    maxb = slots // samples
    peers = lax.axis_size("dp")
    mp = lax.axis_size("mp")
    features, hidden = mid_weight.shape
    pair_cap = (slots + peers - 1) // peers
    per_pair = (pair_cap + mp - 1) // mp
    total = peers * per_pair
    share = (slots + 2 * mp - 1) // (2 * mp)
    owner_rows = 3 * samples
    params = functools.partial(pltpu.CompilerParams, vmem_limit_bytes=48 * 1024 * 1024)
    step = next(features // n for n in (3, 2, 1) if features % (128 * n) == 0 or n == 1)

    send, combined, embed, block_x, block_n, picks, info = pl.pallas_call(
        functools.partial(start_kernel, maxb, per_pair, peers, mp, step),
        in_specs=[HBM] * 11,
        out_specs=[ANY] + [VMEM] * 6,
        out_shape=[
            jax.ShapeDtypeStruct((peers, per_pair * channels + META, width), BF16),
            jax.ShapeDtypeStruct((2 * channels, hidden), BF16),
            jax.ShapeDtypeStruct((channels, features), BF16),
            jax.ShapeDtypeStruct((share, channels, 2 * width), BF16),
            jax.ShapeDtypeStruct((share, channels, 2 * width), BF16),
            jax.ShapeDtypeStruct((2 * share, LANES), jnp.int32),
            jax.ShapeDtypeStruct((META, LANES), F32),
        ],
        scratch_shapes=[
            pltpu.SMEM((samples,), jnp.int32),
            pltpu.SMEM((slots,), jnp.int32),
            pltpu.SMEM((slots,), jnp.int32),
            pltpu.SMEM((samples,), jnp.int32),
            pltpu.SMEM((samples,), F32),
            pltpu.VMEM((1, features), F32),
            pltpu.VMEM((features, hidden), BF16),
            pltpu.VMEM((slots, channels, width), BF16),
            pltpu.VMEM((peers, META, width), BF16),
            pltpu.SMEM((peers + 1,), jnp.int32),
            pltpu.SMEM((total + 1,), jnp.int32),
            pltpu.SMEM((total + 1,), jnp.int32),
            pltpu.SMEM((2 * share + 1,), jnp.int32),
            pltpu.SMEM((2 * share + 1,), jnp.int32),
            pltpu.SemaphoreType.DMA((5,)),
            pltpu.SemaphoreType.DMA((4,)),
            pltpu.SemaphoreType.DMA((features // step,)),
            pltpu.SemaphoreType.DMA((total,)),
            pltpu.SemaphoreType.DMA((2 * share,)),
            pltpu.SemaphoreType.DMA,
        ],
        compiler_params=params(),
        name="start",
    )(
        *map(
            in_hbm,
            (
                frames,
                owners,
                offsets,
                groups,
                rewards,
                latent,
                noise_blocks,
                embed_weight,
                norm_gain.reshape(1, features),
                mid_weight,
                head_weight.T,
            ),
        )
    )

    def swapped(value, axis, count, bit):
        return lax.ppermute(value, axis, [(j, j ^ bit) for j in range(count)])

    recv = lax.all_to_all(send, "dp", split_axis=0, concat_axis=0, tiled=True)
    heads = [combined, swapped(combined, "mp", mp, mp // 2)]
    for n in range(1, mp // 2):
        heads += [swapped(head, "mp", mp, n) for head in heads[:2]]
    near = 2

    partial, halves, mt_near, gram = pl.pallas_call(
        functools.partial(early_kernel, near, features),
        in_specs=[VMEM] * (2 + near),
        out_specs=[VMEM] * 4,
        out_shape=[
            jax.ShapeDtypeStruct((share, channels, 2 * width), F32),
            jax.ShapeDtypeStruct((share, 1, 2 * width), F32),
            jax.ShapeDtypeStruct((near * hidden, 2 * channels), BF16),
            jax.ShapeDtypeStruct((3 * channels, channels), BF16),
        ],
        compiler_params=params(),
        name="early",
    )(block_x, embed, *heads[:near])

    errs, mt_far = pl.pallas_call(
        functools.partial(errors_kernel, mp - near),
        in_specs=[VMEM] * (5 + mp - near),
        out_specs=[VMEM, VMEM],
        out_shape=[
            jax.ShapeDtypeStruct((1, LANES), F32),
            jax.ShapeDtypeStruct(((mp - near) * hidden, 2 * channels), BF16),
        ],
        compiler_params=params(),
        name="errors",
    )(picks, block_x, block_n, partial, halves, *heads[near:])

    tail = (peers + META - 1) // META * META + META
    payload = pl.pallas_call(
        functools.partial(owner_kernel, per_pair, near, mp, features),
        in_specs=[VMEM] * (5 + mp),
        out_specs=VMEM,
        out_shape=jax.ShapeDtypeStruct((total * channels + tail, width), BF16),
        scratch_shapes=[pltpu.SMEM((total + 1,), jnp.int32)],
        compiler_params=params(),
        name="owner",
    )(recv, errs, gram, mt_near, mt_far, *heads)

    gathered = lax.all_gather(payload, "mp", axis=0, tiled=False)

    return pl.pallas_call(
        functools.partial(place_kernel, per_pair, samples),
        in_specs=[VMEM] * 3,
        out_specs=[ANY] * 3,
        out_shape=[
            jax.ShapeDtypeStruct((owner_rows, channels, width), BF16),
            jax.ShapeDtypeStruct((samples,), F32),
            jax.ShapeDtypeStruct((samples,), F32),
        ],
        scratch_shapes=[
            pltpu.SMEM((samples,), F32),
            pltpu.SMEM((samples,), F32),
            pltpu.SemaphoreType.DMA((2,)),
            pltpu.SemaphoreType.DMA,
        ],
        compiler_params=params(),
        name="place",
    )(info, recv, gathered)


def solution(mesh):
    placed = (
        P("dp"),
        P("dp"),
        P("dp"),
        P("dp"),
        P("dp", None, None),
        P("dp", None, None),
        P("dp"),
        P(),
        P(),
        P(None, "mp"),
        P("mp", None),
    )
    return jax.shard_map(
        local,
        mesh=mesh,
        in_specs=placed,
        out_specs=(P("dp", None, None), P("dp"), P("dp")),
        check_vma=False,
    )
```
